512 devices in a mesh: sub: 32 (over x_lo, y, core), dir: 16 (over x_hi, z).
Axes of the slice: x: 4 (x_hi: 2, x_lo: 2; x = x_hi * 2 + x_lo), y: 8, z: 8, core: 2. Of those that a mesh axis runs over, the one named last changes fastest.
Arguments:
- fine_fields: float32 [32768, 2, 1024], P(('sub', 'dir')), may hold values from -6 to 6
- fine_octant: int32 [32768], P(('sub', 'dir')), may hold values from 0 to 7, as said below
- mid_octant: int32 [4096], P('sub'), may hold values from 0 to 7, as said below
- shift_fine: float32 [8, 4096], replicated, may hold values from -3.140625 to 3.140625
- shift_mid: float32 [8, 16384], replicated, may hold values from -3.140625 to 3.140625
- interp_theta_mid: float32 [64, 32], replicated, may hold values from -1 to 1
- interp_phi_mid: float32 [64, 32], replicated, may hold values from -1 to 1
- interp_theta_top: float32 [128, 64], replicated, may hold values from -0.75 to 0.75
- interp_phi_top: float32 [128, 64], replicated, may hold values from -0.75 to 0.75
- partners: int32 [512, 32], P('sub'), may hold values from 0 to 511, as said below
- translation: float32 [512, 32, 2, 16384], P('sub', None, None, 'dir'), may hold values from -0.0234375 to 0.0234375
Outputs:
- fine_incoming: float32 [32768, 2, 1024], P(('sub', 'dir'))
The draws below stay inside these ranges and needn't reach their ends.
Inputs may be any that keep to these rules, and one draw needn't show every extreme that they name: `fine_octant`: each aligned group of 8 entries is a permutation of 0 to 7. `mid_octant`: each aligned group of 8 entries is a permutation of 0 to 7. `partners`: row t names 32 different top boxes, none of them t.
All inputs are finite; a program needn't handle non-finite values.
Results may differ from the reference program's by a relative error of at most 0.000096.
Values sent between devices are 32-bit elements; how exact they have to be, the bound alone decides.
No kernel may reach another device: no remote copies, remote signals or barrier semaphores. Data moves between devices by JAX's collectives and lax.ppermute only.
A program may use at most 64 MiB of HBM per device.

```python
import jax
import jax.numpy as jnp
from jax import lax

THETA_FINE = 32
PHI_FINE = 32
THETA_MID = 64
PHI_MID = 64
THETA_TOP = 128
PHI_TOP = 128
PARTNERS = 32
TOP = 512
MID = 4096
FINE = 32768
DIRS_FINE = 1024
DIRS_MID = 4096
DIRS_TOP = 16384


def octant_perm(key, groups):
    scores = jax.random.randint(key, (groups, 8), 0, 2 ** 20) * 8 + jnp.arange(8, dtype=jnp.int32)[None, :]
    return jnp.argsort(scores, axis=1, stable=True).astype(jnp.int32).reshape(-1)


def draw_fine_octant(key, part):
    return octant_perm(jax.random.fold_in(key, 11), MID)


def draw_mid_octant(key, part):
    return octant_perm(jax.random.fold_in(key, 12), TOP)


def draw_partners(key, part):
    scores = jax.random.randint(jax.random.fold_in(key, 13), (TOP, TOP), 0, 2 ** 16) * TOP
    scores = scores + jnp.arange(TOP, dtype=jnp.int32)[None, :]
    diagonal_mask = jnp.arange(TOP)[:, None] == jnp.arange(TOP)[None, :]
    scores = jnp.where(diagonal_mask, 2 ** 30, scores)
    return jnp.argsort(scores, axis=1, stable=True)[:, :PARTNERS].astype(jnp.int32)


def shard_levels(key, shape, pieces, low, high):
    factor_of, own = 1.0, jax.random.fold_in(key, 6)
    for dim, parts in pieces:
        draws = jnp.exp(jax.random.uniform(jax.random.fold_in(own, dim), (parts,), jnp.float32, low / len(pieces), high / len(pieces)))
        factor_of = factor_of * jnp.repeat(draws, shape[dim] // parts).reshape([-1 if axis == dim else 1 for axis in range(len(shape))])
    return factor_of


def normal_values(stream_key, shape, scale, reach, cuts=(), held_as=jnp.bfloat16):
    gain = shard_levels(stream_key, shape, cuts, -0.22, 0.18) if cuts else 1.0
    array = jax.random.normal(stream_key, shape, jnp.float32) * scale * gain
    return jnp.minimum(jnp.maximum(array, -reach), reach).astype(held_as)


def setup_inputs(seed: int = 0) -> dict:
    streams_of = jax.random.split(jax.random.key(seed), 12)
    return {
        "fine_fields": normal_values(streams_of[0], (FINE, 2, DIRS_FINE), 1.0, 6.0, ((0, 512),), jnp.float32),
        "fine_octant": draw_fine_octant(jax.random.fold_in(streams_of[11], 71), 0),
        "mid_octant": draw_mid_octant(jax.random.fold_in(streams_of[11], 71), 0),
        "shift_fine": jnp.clip(jax.random.uniform(streams_of[3], (8, DIRS_MID), jnp.float32, -3.140625, 3.140625), -3.140625, 3.140625),
        "shift_mid": jnp.clip(jax.random.uniform(streams_of[4], (8, DIRS_TOP), jnp.float32, -3.140625, 3.140625), -3.140625, 3.140625),
        "interp_theta_mid": normal_values(streams_of[5], (THETA_MID, THETA_FINE), THETA_FINE ** -0.5, 1.0, (), jnp.float32),
        "interp_phi_mid": normal_values(streams_of[6], (PHI_MID, PHI_FINE), PHI_FINE ** -0.5, 1.0, (), jnp.float32),
        "interp_theta_top": normal_values(streams_of[7], (THETA_TOP, THETA_MID), THETA_MID ** -0.5, 0.75, (), jnp.float32),
        "interp_phi_top": normal_values(streams_of[8], (PHI_TOP, PHI_MID), PHI_MID ** -0.5, 0.75, (), jnp.float32),
        "partners": draw_partners(jax.random.fold_in(streams_of[11], 71), 0),
        "translation": normal_values(streams_of[10], (TOP, PARTNERS, 2, DIRS_TOP), (1.0 / (8 * PARTNERS)), 0.0234375, ((0, 32), (3, 16)), jnp.float32),
    }


def interpolate(fields, theta_matrix, phi_matrix, theta_count, phi_count):
    boxes = fields.shape[0]
    grid = fields.reshape(boxes, 2, theta_count, phi_count)
    result = jnp.einsum("ta,bcap,fp->bctf", theta_matrix, grid, phi_matrix, precision=lax.Precision.HIGHEST)
    return result.reshape(boxes, 2, -1)


def anterpolate(fields, theta_matrix, phi_matrix):
    boxes = fields.shape[0]
    grid = fields.reshape(boxes, 2, theta_matrix.shape[0], phi_matrix.shape[0])
    result = jnp.einsum("ta,bctf,fp->bcap", theta_matrix, grid, phi_matrix, precision=lax.Precision.HIGHEST)
    return result.reshape(boxes, 2, -1)


def rotate(fields, angles, orient):
    cosine = jnp.cos(angles)
    sine = orient * jnp.sin(angles)
    real_part = fields[:, 0] * cosine - fields[:, 1] * sine
    imag_part = fields[:, 0] * sine + fields[:, 1] * cosine
    return jnp.stack([real_part, imag_part], axis=1)


def reference(fine_fields, fine_octant, mid_octant, shift_fine, shift_mid, interp_theta_mid, interp_phi_mid, interp_theta_top, interp_phi_top, partners, translation):
    fine_angles = shift_fine[fine_octant]
    mid_angles = shift_mid[mid_octant]
    child_mid = rotate(interpolate(fine_fields, interp_theta_mid, interp_phi_mid, THETA_FINE, PHI_FINE), fine_angles, 1.0)
    mid_fields = child_mid.reshape(MID, 8, 2, DIRS_MID).sum(axis=1)
    child_top = rotate(interpolate(mid_fields, interp_theta_top, interp_phi_top, THETA_MID, PHI_MID), mid_angles, 1.0)
    top_fields = child_top.reshape(TOP, 8, 2, DIRS_TOP).sum(axis=1)

    def one_box(inputs):
        listed, operator = inputs
        picked = top_fields[listed]
        real_part = picked[:, 0] * operator[:, 0] - picked[:, 1] * operator[:, 1]
        imag_part = picked[:, 0] * operator[:, 1] + picked[:, 1] * operator[:, 0]
        return jnp.stack([real_part.sum(axis=0), imag_part.sum(axis=0)], axis=0)

    top_incoming = lax.map(one_box, (partners, translation))
    parent_top = jnp.repeat(top_incoming, 8, axis=0)
    mid_incoming = anterpolate(rotate(parent_top, mid_angles, -1.0), interp_theta_top, interp_phi_top)
    parent_mid = jnp.repeat(mid_incoming, 8, axis=0)
    return anterpolate(rotate(parent_mid, fine_angles, -1.0), interp_theta_mid, interp_phi_mid)
```

```python
import jax
import jax.numpy as jnp
from jax import lax
from jax.experimental import pallas as pl
from jax.experimental.pallas import tpu as pltpu
from jax.sharding import PartitionSpec as P

F32 = jnp.float32
BF16 = jnp.bfloat16
VMEM = pl.BlockSpec(memory_space=pltpu.VMEM)
SMEM = pl.BlockSpec(memory_space=pltpu.SMEM)
ANY = pl.BlockSpec(memory_space=pl.ANY)


def split(x):
    high = x.astype(BF16)
    return high, (x - high.astype(F32)).astype(BF16)


def dot(a, b, dims=((1,), (0,))):
    return lax.dot_general(a, b, (dims, ((), ())), preferred_element_type=F32)


def onehot(shape, source):
    rows = lax.broadcasted_iota(jnp.int32, shape, 0)
    cols = lax.broadcasted_iota(jnp.int32, shape, 1)
    return jnp.where(source(rows, cols), 1.0, 0.0).astype(BF16)


def cos_sin(angles):
    half = angles * 0.5
    square = half * half
    sine = -1.0 / 39916800.0
    for term in (1.0 / 362880.0, -1.0 / 5040.0, 1.0 / 120.0, -1.0 / 6.0, 1.0):
        sine = sine * square + term
    sine = sine * half
    cosine = 1.0 / 479001600.0
    for term in (-1.0 / 3628800.0, 1.0 / 40320.0, -1.0 / 720.0, 1.0 / 24.0, -0.5, 1.0):
        cosine = cosine * square + term
    return 1.0 - 2.0 * (sine * sine), 2.0 * (sine * cosine)


def group_transpose(v):
    lane = lax.broadcasted_iota(jnp.int32, v[0].shape, 1)
    low = lane < 64
    even = (lane // 32) % 2 == 0
    roll = lambda x, by: pltpu.roll(x, by, 1)
    x0 = jnp.where(low, v[0], roll(v[2], 64))
    x2 = jnp.where(low, roll(v[0], 64), v[2])
    x1 = jnp.where(low, v[1], roll(v[3], 64))
    x3 = jnp.where(low, roll(v[1], 64), v[3])
    return [
        jnp.where(even, x0, roll(x1, 32)),
        jnp.where(even, roll(x0, 96), x1),
        jnp.where(even, x2, roll(x3, 32)),
        jnp.where(even, roll(x2, 96), x3),
    ]


def invert(octants, inverse, count):
    def step(i, _):
        inverse[(i // 8) * 8 + octants[i]] = i
        return 0

    lax.fori_loop(0, count, step, 0, unroll=8)


def fine_tables(angle_ref, cos_ref, sin_ref):
    for pair in range(4):
        first = angle_ref[pl.ds(2 * pair, 32, stride=8), :]
        second = angle_ref[pl.ds(2 * pair + 1, 32, stride=8), :]
        low = lax.broadcasted_iota(jnp.int32, first.shape, 1) < 64
        for odd, angles in enumerate(
            (
                jnp.where(low, first, pltpu.roll(second, 64, 1)),
                jnp.where(low, pltpu.roll(first, 64, 1), second),
            )
        ):
            cosine, sine = cos_sin(angles)
            cos_ref[pair, pl.ds(32 * odd, 32), :] = cosine
            sin_ref[pair, pl.ds(32 * odd, 32), :] = sine


def top_tables(angle_ref, cos_ref, sin_ref):
    for i in range(16):
        cosine, sine = cos_sin(angle_ref[pl.ds(64 * i, 64), :])
        cos_ref[pl.ds(64 * i, 64), :] = cosine
        sin_ref[pl.ds(64 * i, 64), :] = sine


def block_diagonal(matrix, copies):
    n, k = matrix.shape
    spread = onehot((k, copies * k), lambda r, c: c % k == r)
    out = []
    for part in split(matrix):
        wide = dot(part, spread)
        tall = jnp.concatenate([wide] * copies, axis=0)
        rows = lax.broadcasted_iota(jnp.int32, tall.shape, 0) // n
        cols = lax.broadcasted_iota(jnp.int32, tall.shape, 1) // k
        out.append(jnp.where(rows == cols, tall, 0.0).astype(BF16))
    return out


def up_kernel(
    fine, fine_oct, mid_oct, angle_fine, angle_mid, theta_mid, phi_mid, theta_top, phi_top,
    out, fine_inv, mid_inv, cos_f, sin_f, cos_t, sin_t, mids,
):
    invert(fine_oct, fine_inv, 64)
    invert(mid_oct, mid_inv, 8)
    fine_tables(angle_fine, cos_f, sin_f)
    top_tables(angle_mid, cos_t, sin_t)
    a_rows = jnp.concatenate(
        [theta_mid[pl.ds(0, 32, stride=2), :], theta_mid[pl.ds(1, 32, stride=2), :]], axis=0
    )
    a_high, a_low = split(a_rows)
    pick = lambda r, c: r == 4 * ((c % 32) % 8) + (c % 32) // 8
    a_mid = (
        dot(a_high, onehot((32, 96), lambda r, c: pick(r, c) & (c < 64)))
        + dot(a_low, onehot((32, 96), lambda r, c: pick(r, c) & (c >= 64)))
    ).astype(BF16)
    b_high, b_low = block_diagonal(phi_mid[...], 4)
    b_mid = jnp.concatenate([b_high, b_high, b_low], axis=1)
    a_high, a_low = split(theta_top[...])
    pick_top = lambda r, c: r == 2 * ((c % 64) % 32) + (c % 64) // 32
    a_top = (
        dot(a_high, onehot((64, 192), lambda r, c: pick_top(r, c) & (c < 128)))
        + dot(a_low, onehot((64, 192), lambda r, c: pick_top(r, c) & (c >= 128)))
    ).astype(BF16)
    b_high, b_low = block_diagonal(phi_top[...], 2)
    b_top = jnp.concatenate([b_high, b_high, b_low], axis=1)
    for octant in range(8):
        m = mid_inv[octant]
        chunks = []
        for h in range(2):
            boxes = [fine_inv[m * 8 + 4 * h + b] for b in range(4)]
            for c in range(2):
                v = [fine[box, pl.ds(c, 8, stride=2), :] for box in boxes]
                chunks.append(jnp.concatenate(group_transpose(v), axis=0))
        w_high, w_low = split(jnp.concatenate(chunks, axis=1))
        y = dot(a_mid, jnp.concatenate([w_high, w_low, w_high], axis=0))
        y = jnp.concatenate([y[:, 128 * i : 128 * i + 128] for i in range(4)], axis=0)
        y_high, y_low = split(y)
        z = dot(jnp.concatenate([y_high, y_low, y_high], axis=1), b_mid, ((1,), (1,)))
        real, imag = 0.0, 0.0
        for h in range(2):
            for j in range(2):
                re = z[128 * h : 128 * h + 64, 128 * j : 128 * j + 128]
                im = z[128 * h + 64 : 128 * h + 128, 128 * j : 128 * j + 128]
                cosine, sine = cos_f[2 * h + j], sin_f[2 * h + j]
                real = real + (re * cosine - im * sine)
                imag = imag + (re * sine + im * cosine)
        mids[octant, 0] = real + pltpu.roll(real, 64, 1)
        mids[octant, 1] = imag + pltpu.roll(imag, 64, 1)
    low = lax.broadcasted_iota(jnp.int32, (64, 128), 1) < 64
    top = [0.0, 0.0]
    for pair in range(4):
        chunks = [
            jnp.where(low, mids[2 * pair, c], mids[2 * pair + 1, c]) for c in range(2)
        ]
        w_high, w_low = split(jnp.concatenate(chunks, axis=1))
        y = dot(a_top, jnp.concatenate([w_high, w_low, w_high], axis=0))
        y = jnp.concatenate([y[:, :128], y[:, 128:]], axis=0)
        y_high, y_low = split(y)
        z = dot(jnp.concatenate([y_high, y_low, y_high], axis=1), b_top, ((1,), (1,)))
        for j in range(2):
            re = z[:128, 128 * j : 128 * j + 128]
            im = z[128:, 128 * j : 128 * j + 128]
            cosine = cos_t[pl.ds(2 * pair + j, 128, stride=8), :]
            sine = sin_t[pl.ds(2 * pair + j, 128, stride=8), :]
            top[0] = top[0] + (re * cosine - im * sine)
            top[1] = top[1] + (re * sine + im * cosine)
    for c in range(2):
        for d in range(16):
            out[d, pl.ds(8 * c, 8), :] = top[c][8 * d : 8 * d + 8]


def down_kernel(
    parent, fine_oct, mid_oct, angle_fine, angle_mid, theta_mid, phi_mid, theta_top, phi_top,
    out, fine_inv, mid_inv, cos_f, sin_f, cos_t, sin_t,
):
    invert(fine_oct, fine_inv, 64)
    invert(mid_oct, mid_inv, 8)
    fine_tables(angle_fine, cos_f, sin_f)
    top_tables(angle_mid, cos_t, sin_t)
    spread = onehot((64, 128), lambda r, c: c % 64 == r)
    b_high, b_low = [dot(part, spread).astype(BF16) for part in split(phi_top[...])]
    b_top = jnp.concatenate([b_high, b_high, b_low], axis=0)
    order = onehot((64, 64), lambda r, c: c == 2 * (r % 32) + r // 32)
    a_high, a_low = [
        dot(order, part, ((1,), (1,))).astype(BF16) for part in split(theta_top[...])
    ]
    a_top = jnp.concatenate([a_high, a_high, a_low], axis=1)
    b_high, b_low = block_diagonal(phi_mid[...], 4)
    b_mid = jnp.concatenate([b_high, b_high, b_low], axis=0)
    a_rows = jnp.concatenate(
        [theta_mid[pl.ds(0, 32, stride=2), :], theta_mid[pl.ds(1, 32, stride=2), :]], axis=0
    )
    a_high, a_low = split(a_rows)
    order = onehot((32, 32), lambda r, c: c == 4 * (r % 8) + r // 8)
    a_mid = dot(
        order, jnp.concatenate([a_high, a_high, a_low], axis=0), ((1,), (1,))
    ).astype(BF16)
    field = [
        jnp.concatenate([parent[d, pl.ds(8 * c, 8), :] for d in range(16)], axis=0)
        for c in range(2)
    ]
    for octant in range(8):
        m = mid_inv[octant]
        cosine = cos_t[pl.ds(octant, 128, stride=8), :]
        sine = sin_t[pl.ds(octant, 128, stride=8), :]
        x = jnp.concatenate(
            [field[0] * cosine + field[1] * sine, field[1] * cosine - field[0] * sine], axis=0
        )
        x_high, x_low = split(x)
        y = dot(jnp.concatenate([x_high, x_low, x_high], axis=1), b_top)
        y_high, y_low = split(jnp.concatenate([y[:128], y[128:]], axis=1))
        mid = dot(a_top, jnp.concatenate([y_high, y_low, y_high], axis=0))
        re, im = mid[:, :128], mid[:, 128:]
        chunks = []
        for h in range(2):
            c0, s0 = cos_f[2 * h], sin_f[2 * h]
            c1, s1 = cos_f[2 * h + 1], sin_f[2 * h + 1]
            chunks.append(jnp.concatenate([re * c0 + im * s0, re * c1 + im * s1], axis=1))
            chunks.append(jnp.concatenate([im * c0 - re * s0, im * c1 - re * s1], axis=1))
        x_high, x_low = split(jnp.concatenate(chunks, axis=0))
        y = dot(jnp.concatenate([x_high, x_low, x_high], axis=1), b_mid)
        y = jnp.concatenate([y[64 * i : 64 * i + 64] for i in range(4)], axis=1)
        y_high, y_low = split(y)
        w = dot(a_mid, jnp.concatenate([y_high, y_low, y_high], axis=0))
        for h in range(2):
            boxes = [fine_inv[m * 8 + 4 * h + b] for b in range(4)]
            for c in range(2):
                lanes = 128 * (2 * h + c)
                v = group_transpose(
                    [w[8 * g : 8 * g + 8, lanes : lanes + 128] for g in range(4)]
                )
                for b in range(4):
                    out[boxes[b], pl.ds(c, 8, stride=2), :] = v[b]


def tables_scratch():
    return [
        pltpu.SMEM((64,), jnp.int32),
        pltpu.SMEM((8,), jnp.int32),
        pltpu.VMEM((4, 64, 128), F32),
        pltpu.VMEM((4, 64, 128), F32),
        pltpu.VMEM((1024, 128), F32),
        pltpu.VMEM((1024, 128), F32),
    ]


def call_up(fine, fine_oct, mid_oct, angle_fine, angle_mid, matrices):
    return pl.pallas_call(
        up_kernel,
        out_shape=jax.ShapeDtypeStruct((16, 16, 128), F32),
        in_specs=[VMEM, SMEM, SMEM] + [VMEM] * 6,
        out_specs=VMEM,
        scratch_shapes=tables_scratch() + [pltpu.VMEM((8, 2, 64, 128), F32)],
        name="upward",
    )(fine, fine_oct, mid_oct, angle_fine, angle_mid, *matrices)


def call_down(parent, fine_oct, mid_oct, angle_fine, angle_mid, matrices):
    return pl.pallas_call(
        down_kernel,
        out_shape=jax.ShapeDtypeStruct((64, 16, 128), F32),
        in_specs=[VMEM, SMEM, SMEM] + [VMEM] * 6,
        out_specs=VMEM,
        scratch_shapes=tables_scratch(),
        name="downward",
    )(parent, fine_oct, mid_oct, angle_fine, angle_mid, *matrices)


def translate_kernel(slots, translation, *refs):
    pieces, out, fields, sems = refs[:-3], refs[-3], refs[-2], refs[-1]
    t = pl.program_id(0)

    @pl.when(t == 0)
    def _():
        copies, start = [], 0
        for i, piece in enumerate(pieces):
            count = piece.shape[0]
            copies.append(
                pltpu.make_async_copy(piece, fields.at[pl.ds(start, count)], sems.at[i])
            )
            start += count
        for copy in copies:
            copy.start()
        for copy in copies:
            copy.wait()

    real = [0.0] * 4
    imag = [0.0] * 4
    for k in range(32):
        n = slots[t, k]
        fr, fi = fields[n, pl.ds(0, 8), :], fields[n, pl.ds(8, 8), :]
        tr = translation[k, pl.ds(0, 8, stride=2), :]
        ti = translation[k, pl.ds(1, 8, stride=2), :]
        real[k % 4] = real[k % 4] + (fr * tr - fi * ti)
        imag[k % 4] = imag[k % 4] + (fr * ti + fi * tr)
    out[0, pl.ds(0, 8), :] = (real[0] + real[1]) + (real[2] + real[3])
    out[0, pl.ds(8, 8), :] = (imag[0] + imag[1]) + (imag[2] + imag[3])


def call_translate(slots, translation, pieces):
    return pl.pallas_call(
        translate_kernel,
        grid=(16,),
        out_shape=jax.ShapeDtypeStruct((16, 16, 128), F32),
        in_specs=[SMEM, pl.BlockSpec((32, 16, 128), lambda t: (t, 0, 0))] + [ANY] * len(pieces),
        out_specs=pl.BlockSpec((1, 16, 128), lambda t: (t, 0, 0)),
        scratch_shapes=[
            pltpu.VMEM((512, 16, 128), F32),
            pltpu.SemaphoreType.DMA((len(pieces),)),
        ],
        name="translate",
    )(slots, translation, *pieces)


def permutations():
    place = lambda x, y, core: x * 16 + (y % 8) * 2 + core
    every = [(x, y, core) for x in range(2) for y in range(8) for core in range(2)]
    shift = lambda by: [(place(x, y, c), place(x, y + by, c)) for x, y, c in every]
    across = [(place(x, y, c), place(1 - x, y, c)) for x, y, c in every]
    other = [(place(x, y, c), place(x, y, 1 - c)) for x, y, c in every]
    return shift(1), shift(-1), across, other


def gather_tops(top_fields):
    ahead, behind, across, other = permutations()
    send = lambda x, perm: lax.ppermute(x, "sub", perm)
    own = jnp.concatenate([top_fields, send(top_fields, across)], axis=0)
    up, down = [], []
    forward = backward = own
    for _ in range(3):
        forward, backward = send(forward, ahead), send(backward, behind)
        up.append(backward)
        down.append(forward)
    half = own.shape[0] // 2
    fourth = [send(forward[:half], ahead), send(backward[half:], behind)]
    mine = [own] + up + fourth + down[::-1]
    partner = send(jnp.concatenate(mine, axis=0), other)
    return mine + [partner]


def slot_of(boxes, my_sub):
    sub, slot = boxes // 16, boxes % 16
    rise = (sub // 2 - my_sub // 2) % 8
    far_x = (sub // 16 != my_sub // 16).astype(jnp.int32)
    far_core = (sub % 2 != my_sub % 2).astype(jnp.int32)
    return far_core * 256 + rise * 32 + far_x * 16 + slot


def body(
    fine_fields,
    fine_octant,
    mid_octant,
    shift_fine,
    shift_mid,
    interp_theta_mid,
    interp_phi_mid,
    interp_theta_top,
    interp_phi_top,
    partners,
    translation,
):
    my_dir = lax.axis_index("dir")
    my_sub = lax.axis_index("sub")
    my_octants = lax.dynamic_slice_in_dim(mid_octant, my_dir * 8, 8)
    fine = fine_fields.reshape(64, 2, 8, 128).transpose(0, 2, 1, 3).reshape(64, 16, 128)
    operator = translation.reshape(512, 2, 8, 128).transpose(0, 2, 1, 3).reshape(512, 16, 128)
    angle_fine = shift_fine.reshape(8, 32, 128).transpose(1, 0, 2).reshape(256, 128)
    angle_mid = shift_mid.reshape(8, 128, 128).transpose(1, 0, 2).reshape(1024, 128)
    matrices = (interp_theta_mid, interp_phi_mid, interp_theta_top, interp_phi_top)
    slots = slot_of(partners, my_sub)
    top = call_up(fine, fine_octant, my_octants, angle_fine, angle_mid, matrices)
    top_fields = lax.all_to_all(top, "dir", split_axis=0, concat_axis=0, tiled=True)
    pieces = gather_tops(top_fields)
    incoming = call_translate(slots, operator, pieces)
    parent = lax.all_to_all(incoming, "dir", split_axis=0, concat_axis=0, tiled=True)
    result = call_down(parent, fine_octant, my_octants, angle_fine, angle_mid, matrices)
    return result.reshape(64, 8, 2, 128).transpose(0, 2, 1, 3).reshape(64, 2, 1024)


def solution(mesh):
    in_specs = (
        P(("sub", "dir"), None, None),
        P(("sub", "dir")),
        P("sub"),
        P(),
        P(),
        P(),
        P(),
        P(),
        P(),
        P("sub", None),
        P("sub", None, None, "dir"),
    )
    out_specs = P(("sub", "dir"), None, None)
    return jax.shard_map(body, mesh=mesh, in_specs=in_specs, out_specs=out_specs, check_vma=False)
```

```python
import jax
import jax.numpy as jnp
from jax import lax
from jax.experimental import pallas as pl
from jax.experimental.pallas import tpu as pltpu
from jax.sharding import PartitionSpec as P

F32 = jnp.float32
BF16 = jnp.bfloat16
VMEM = pl.BlockSpec(memory_space=pltpu.VMEM)
SMEM = pl.BlockSpec(memory_space=pltpu.SMEM)
UP_GROUP, TOP_GROUP, DOWN_GROUP = 4, 2, 4
ANY = pl.BlockSpec(memory_space=pl.ANY)


def split(x):
    high = x.astype(BF16)
    return high, (x - high.astype(F32)).astype(BF16)


def dot(a, b, dims=((1,), (0,))):
    return lax.dot_general(a, b, (dims, ((), ())), preferred_element_type=F32)


def onehot(shape, source):
    rows = lax.broadcasted_iota(jnp.int32, shape, 0)
    cols = lax.broadcasted_iota(jnp.int32, shape, 1)
    return jnp.where(source(rows, cols), 1.0, 0.0).astype(BF16)


def cos_sin(angles):
    half = angles * 0.5
    square = half * half
    sine = -1.0 / 39916800.0
    for term in (1.0 / 362880.0, -1.0 / 5040.0, 1.0 / 120.0, -1.0 / 6.0, 1.0):
        sine = sine * square + term
    sine = sine * half
    cosine = 1.0 / 479001600.0
    for term in (-1.0 / 3628800.0, 1.0 / 40320.0, -1.0 / 720.0, 1.0 / 24.0, -0.5, 1.0):
        cosine = cosine * square + term
    return 1.0 - 2.0 * (sine * sine), 2.0 * (sine * cosine)


def group_transpose(v):
    lane = lax.broadcasted_iota(jnp.int32, v[0].shape, 1)
    low = lane < 64
    even = (lane // 32) % 2 == 0
    roll = lambda x, by: pltpu.roll(x, by, 1)
    x0 = jnp.where(low, v[0], roll(v[2], 64))
    x2 = jnp.where(low, roll(v[0], 64), v[2])
    x1 = jnp.where(low, v[1], roll(v[3], 64))
    x3 = jnp.where(low, roll(v[1], 64), v[3])
    return [
        jnp.where(even, x0, roll(x1, 32)),
        jnp.where(even, roll(x0, 96), x1),
        jnp.where(even, x2, roll(x3, 32)),
        jnp.where(even, roll(x2, 96), x3),
    ]


def invert(octants, inverse, count, first):
    def step(i, _):
        inverse[(i // 8) * 8 + octants[first + i]] = i
        return 0

    lax.fori_loop(0, count, step, 0, unroll=8)


def fine_tables(angle_ref, cos_ref, sin_ref):
    for pair in range(4):
        first = angle_ref[pl.ds(2 * pair, 32, stride=8), :]
        second = angle_ref[pl.ds(2 * pair + 1, 32, stride=8), :]
        low = lax.broadcasted_iota(jnp.int32, first.shape, 1) < 64
        for odd, angles in enumerate(
            (
                jnp.where(low, first, pltpu.roll(second, 64, 1)),
                jnp.where(low, pltpu.roll(first, 64, 1), second),
            )
        ):
            cosine, sine = cos_sin(angles)
            cos_ref[pair, pl.ds(32 * odd, 32), :] = cosine
            sin_ref[pair, pl.ds(32 * odd, 32), :] = sine


def top_tables(angle_ref, cos_ref, sin_ref):
    for i in range(16):
        cosine, sine = cos_sin(angle_ref[pl.ds(64 * i, 64), :])
        cos_ref[pl.ds(64 * i, 64), :] = cosine
        sin_ref[pl.ds(64 * i, 64), :] = sine


def block_diagonal(matrix, copies):
    n, k = matrix.shape
    spread = onehot((k, copies * k), lambda r, c: c % k == r)
    out = []
    for part in split(matrix):
        wide = dot(part, spread)
        tall = jnp.concatenate([wide] * copies, axis=0)
        rows = lax.broadcasted_iota(jnp.int32, tall.shape, 0) // n
        cols = lax.broadcasted_iota(jnp.int32, tall.shape, 1) // k
        out.append(jnp.where(rows == cols, tall, 0.0).astype(BF16))
    return out


def theta_up(theta, rows, cols):
    targets, sources = theta.shape[1], theta.shape[0]
    high, low = [
        dot(onehot((targets, targets), rows), part, ((1,), (1,))).astype(BF16)
        for part in split(theta)
    ]
    wide = (sources, 3 * sources)
    order = lambda r, c: cols(r, c % sources)
    first = onehot(wide, lambda r, c: order(r, c) & (c < 2 * sources))
    last = onehot(wide, lambda r, c: order(r, c) & (c >= 2 * sources))
    return (dot(high, first) + dot(low, last)).astype(BF16)


def theta_down(theta, rows, cols):
    sources, targets = theta.shape
    high, low = [
        dot(onehot((sources, sources), rows), part).astype(BF16) for part in split(theta)
    ]
    wide = (targets, 3 * targets)
    order = lambda r, c: cols(r, c % targets)
    first = onehot(wide, lambda r, c: order(r, c) & (c < 2 * targets))
    last = onehot(wide, lambda r, c: order(r, c) & (c >= 2 * targets))
    return (dot(high, first) + dot(low, last)).astype(BF16)


def up_kernel(
    fine, fine_oct, mid_oct, angle_fine, angle_mid, theta_mid, phi_mid, theta_top, phi_top,
    out, fine_inv, mid_inv, cos_f, sin_f, cos_t, sin_t, mids,
):
    invert(fine_oct, fine_inv, 64, 0)
    invert(mid_oct, mid_inv, 8, lax.axis_index("dir") * 8)
    fine_tables(angle_fine, cos_f, sin_f)
    top_tables(angle_mid, cos_t, sin_t)
    a_mid = theta_up(
        theta_mid[...],
        lambda r, c: c == 2 * (r % 32) + r // 32,
        lambda r, c: r == 4 * (c % 8) + c // 8,
    )
    a_top = theta_up(
        theta_top[...], lambda r, c: r == c, lambda r, c: r == 2 * (c % 32) + c // 32
    )
    b_high, b_low = block_diagonal(phi_mid[...], 4)
    b_mid = jnp.concatenate([b_high, b_high, b_low], axis=0)
    b_high, b_low = block_diagonal(phi_top[...], 2)
    b_top = jnp.concatenate([b_high, b_high, b_low], axis=0)
    for first in range(0, 8, UP_GROUP):
        chunks = []
        for octant in range(first, first + UP_GROUP):
            m = mid_inv[octant]
            for h in range(2):
                boxes = [fine_inv[m * 8 + 4 * h + b] for b in range(4)]
                for c in range(2):
                    v = [fine[box, pl.ds(c, 8, stride=2), :] for box in boxes]
                    chunks.append(jnp.concatenate(group_transpose(v), axis=0))
        w_high, w_low = split(jnp.concatenate(chunks, axis=1))
        y = dot(a_mid, jnp.concatenate([w_high, w_low, w_high], axis=0))
        y = jnp.concatenate([y[:, 128 * i : 128 * i + 128] for i in range(len(chunks))], axis=0)
        y_high, y_low = split(y)
        z = dot(jnp.concatenate([y_high, y_low, y_high], axis=1), b_mid)
        for g in range(UP_GROUP):
            real, imag = 0.0, 0.0
            for h in range(2):
                row = 256 * g + 128 * h
                for j in range(2):
                    re = z[row : row + 64, 128 * j : 128 * j + 128]
                    im = z[row + 64 : row + 128, 128 * j : 128 * j + 128]
                    cosine, sine = cos_f[2 * h + j], sin_f[2 * h + j]
                    real = real + (re * cosine - im * sine)
                    imag = imag + (re * sine + im * cosine)
            mids[first + g, 0] = real + pltpu.roll(real, 64, 1)
            mids[first + g, 1] = imag + pltpu.roll(imag, 64, 1)
    low = lax.broadcasted_iota(jnp.int32, (64, 128), 1) < 64
    top = [0.0, 0.0]
    for first in range(0, 4, TOP_GROUP):
        chunks = [
            jnp.where(low, mids[2 * pair, c], mids[2 * pair + 1, c])
            for pair in range(first, first + TOP_GROUP)
            for c in range(2)
        ]
        w_high, w_low = split(jnp.concatenate(chunks, axis=1))
        y = dot(a_top, jnp.concatenate([w_high, w_low, w_high], axis=0))
        y = jnp.concatenate([y[:, 128 * i : 128 * i + 128] for i in range(len(chunks))], axis=0)
        y_high, y_low = split(y)
        z = dot(jnp.concatenate([y_high, y_low, y_high], axis=1), b_top)
        for g in range(TOP_GROUP):
            for j in range(2):
                re = z[256 * g : 256 * g + 128, 128 * j : 128 * j + 128]
                im = z[256 * g + 128 : 256 * g + 256, 128 * j : 128 * j + 128]
                octant = 2 * (first + g) + j
                cosine = cos_t[pl.ds(octant, 128, stride=8), :]
                sine = sin_t[pl.ds(octant, 128, stride=8), :]
                top[0] = top[0] + (re * cosine - im * sine)
                top[1] = top[1] + (re * sine + im * cosine)
    for c in range(2):
        for d in range(16):
            for x in range(2):
                out[16 * x + d, pl.ds(8 * c, 8), :] = top[c][8 * d : 8 * d + 8]


def prepare_kernel(
    angle_fine, angle_mid, theta_mid, phi_mid, theta_top, phi_top,
    cos_f, sin_f, cos_t, sin_t, a_mid, b_mid, a_top, b_top,
):
    fine_tables(angle_fine, cos_f, sin_f)
    top_tables(angle_mid, cos_t, sin_t)
    b_high, b_low = [jnp.concatenate([part, part], axis=0) for part in split(phi_top[...])]
    b_top[...] = jnp.concatenate([b_high, b_high, b_low], axis=1)
    a_top[...] = theta_down(
        theta_top[...], lambda r, c: c == 2 * (r % 32) + r // 32, lambda r, c: r == c
    )
    b_high, b_low = block_diagonal(phi_mid[...], 4)
    b_mid[...] = jnp.concatenate([b_high, b_high, b_low], axis=1)
    a_mid[...] = theta_down(
        theta_mid[...],
        lambda r, c: c == 4 * (r % 8) + r // 8,
        lambda r, c: r == 2 * (c % 32) + c // 32,
    )


def down_kernel(
    parent, fine_oct, mid_oct, cos_f, sin_f, cos_t, sin_t, a_mid, b_mid, a_top, b_top,
    out, fine_inv, mid_inv,
):
    invert(fine_oct, fine_inv, 64, 0)
    invert(mid_oct, mid_inv, 8, lax.axis_index("dir") * 8)
    field = [
        jnp.concatenate([parent[d, pl.ds(8 * c, 8), :] for d in range(16)], axis=0)
        for c in range(2)
    ]
    across = ((1,), (1,))
    for first in range(0, 8, DOWN_GROUP):
        rows = []
        for octant in range(first, first + DOWN_GROUP):
            cosine = cos_t[pl.ds(octant, 128, stride=8), :]
            sine = sin_t[pl.ds(octant, 128, stride=8), :]
            rows.append(field[0] * cosine + field[1] * sine)
            rows.append(field[1] * cosine - field[0] * sine)
        x_high, x_low = split(jnp.concatenate(rows, axis=0))
        y = dot(jnp.concatenate([x_high, x_low, x_high], axis=1), b_top[...], across)
        y = jnp.concatenate([y[128 * i : 128 * i + 128] for i in range(len(rows))], axis=1)
        y_high, y_low = split(y)
        mid = dot(a_top[...], jnp.concatenate([y_high, y_low, y_high], axis=0))
        rows = []
        for g in range(DOWN_GROUP):
            re, im = mid[:, 256 * g : 256 * g + 128], mid[:, 256 * g + 128 : 256 * g + 256]
            for h in range(2):
                c0, s0 = cos_f[2 * h], sin_f[2 * h]
                c1, s1 = cos_f[2 * h + 1], sin_f[2 * h + 1]
                rows.append(jnp.concatenate([re * c0 + im * s0, re * c1 + im * s1], axis=1))
                rows.append(jnp.concatenate([im * c0 - re * s0, im * c1 - re * s1], axis=1))
        x_high, x_low = split(jnp.concatenate(rows, axis=0))
        y = dot(jnp.concatenate([x_high, x_low, x_high], axis=1), b_mid[...], across)
        y = jnp.concatenate([y[64 * i : 64 * i + 64] for i in range(len(rows))], axis=1)
        y_high, y_low = split(y)
        w = dot(a_mid[...], jnp.concatenate([y_high, y_low, y_high], axis=0))
        for g in range(DOWN_GROUP):
            m = mid_inv[first + g]
            for h in range(2):
                boxes = [fine_inv[m * 8 + 4 * h + b] for b in range(4)]
                for c in range(2):
                    lanes = 128 * (4 * g + 2 * h + c)
                    v = group_transpose(
                        [w[8 * i : 8 * i + 8, lanes : lanes + 128] for i in range(4)]
                    )
                    for b in range(4):
                        out[boxes[b], pl.ds(c, 8, stride=2), :] = v[b]


def in_vmem(x):
    return pltpu.with_memory_space_constraint(x, pltpu.VMEM)


INVERSES = [pltpu.SMEM((64,), jnp.int32), pltpu.SMEM((8,), jnp.int32)]
TABLES = [((4, 64, 128), F32)] * 2 + [((1024, 128), F32)] * 2
DOWN_MATRICES = [((32, 192), BF16), ((128, 768), BF16), ((64, 384), BF16), ((128, 384), BF16)]


def call_up(fine, fine_oct, mid_oct, tables_of):
    return pl.pallas_call(
        up_kernel,
        out_shape=pltpu.VMEM((32, 16, 128), F32),
        in_specs=[VMEM, SMEM, SMEM] + [VMEM] * 6,
        out_specs=VMEM,
        scratch_shapes=INVERSES
        + [pltpu.VMEM(*table) for table in TABLES]
        + [pltpu.VMEM((8, 2, 64, 128), F32)],
        compiler_params=pltpu.CompilerParams(vmem_limit_bytes=20 * 2**20),
        name="upward",
    )(fine, fine_oct, mid_oct, *tables_of)


def call_prepare(tables_of):
    shapes = TABLES + DOWN_MATRICES
    return pl.pallas_call(
        prepare_kernel,
        out_shape=[pltpu.VMEM(*shape) for shape in shapes],
        in_specs=[VMEM] * 6,
        out_specs=[VMEM] * len(shapes),
        cost_estimate=pl.CostEstimate(flops=200000000, bytes_accessed=2000000, transcendentals=0),
        compiler_params=pltpu.CompilerParams(vmem_limit_bytes=12 * 2**20),
        name="prepare",
    )(*tables_of)


def call_down(parent, fine_oct, mid_oct, prepared):
    return pl.pallas_call(
        down_kernel,
        out_shape=jax.ShapeDtypeStruct((64, 16, 128), F32),
        in_specs=[VMEM, SMEM, SMEM] + [VMEM] * 8,
        out_specs=VMEM,
        scratch_shapes=INVERSES,
        compiler_params=pltpu.CompilerParams(vmem_limit_bytes=24 * 2**20),
        name="downward",
    )(in_vmem(parent), fine_oct, mid_oct, *[in_vmem(x) for x in prepared])


def add_pairs(slots, tables, fields, first, t, total):
    real, imag = [total[0]] + [0.0] * 3, [total[1]] + [0.0] * 3
    for k in range(32):
        n = slots[t, k] - first
        inside = jnp.where((n >= 0) & (n < 256), 1.0, 0.0)
        n = jnp.clip(n, 0, 255)
        fr, fi = fields[n, pl.ds(0, 8), :] * inside, fields[n, pl.ds(8, 8), :] * inside
        tr = tables[32 * t + k, pl.ds(0, 8, stride=2), :]
        ti = tables[32 * t + k, pl.ds(1, 8, stride=2), :]
        real[k % 4] = real[k % 4] + (fr * tr - fi * ti)
        imag[k % 4] = imag[k % 4] + (fr * ti + fi * tr)
    return (real[0] + real[1]) + (real[2] + real[3]), (imag[0] + imag[1]) + (imag[2] + imag[3])


def near_kernel(slots, tables, near, out):
    for t in range(16):
        real, imag = add_pairs(slots, tables, near, 0, t, (0.0, 0.0))
        out[t, pl.ds(0, 8), :] = real
        out[t, pl.ds(8, 8), :] = imag


def far_kernel(slots, tables, far, partial, out):
    for t in range(16):
        total = partial[t, pl.ds(0, 8), :], partial[t, pl.ds(8, 8), :]
        real, imag = add_pairs(slots, tables, far, 256, t, total)
        out[t, pl.ds(0, 8), :] = real
        out[t, pl.ds(8, 8), :] = imag


def call_near(slots, tables, near):
    return pl.pallas_call(
        near_kernel,
        out_shape=pltpu.VMEM((16, 16, 128), F32),
        in_specs=[SMEM, VMEM, VMEM],
        out_specs=VMEM,
        cost_estimate=pl.CostEstimate(flops=200000000, bytes_accessed=6000000, transcendentals=0),
        compiler_params=pltpu.CompilerParams(vmem_limit_bytes=6 * 2**20),
        name="near",
    )(slots, in_vmem(tables), in_vmem(near))


def call_far(slots, tables, far, partial):
    return pl.pallas_call(
        far_kernel,
        out_shape=pltpu.VMEM((16, 16, 128), F32),
        in_specs=[SMEM, VMEM, VMEM, VMEM],
        out_specs=VMEM,
        compiler_params=pltpu.CompilerParams(vmem_limit_bytes=6 * 2**20),
        name="far",
    )(slots, in_vmem(tables), in_vmem(far), in_vmem(partial))


def permutations():
    place = lambda x, y, core: x * 16 + (y % 8) * 2 + core
    every = [(x, y, core) for x in range(2) for y in range(8) for core in range(2)]
    shift = lambda by: [(place(x, y, c), place(x, y + by, c)) for x, y, c in every]
    other = [(place(x, y, c), place(x, y, 1 - c)) for x, y, c in every]
    return shift(1), shift(-1), other


def gather_tops(own):
    ahead, behind, other = permutations()
    send = lambda x, perm: lax.ppermute(x, "sub", perm)
    up, down = [], []
    forward = backward = own
    for _ in range(3):
        forward, backward = send(forward, ahead), send(backward, behind)
        up.append(backward)
        down.append(forward)
    half = own.shape[0] // 2
    fourth = [send(forward[:half], ahead), send(backward[half:], behind)]
    mine = [own] + up + fourth + down[::-1]
    near = jnp.concatenate(mine, axis=0)
    return near, send(near, other)


def slot_of(boxes, my_sub):
    sub, slot = boxes // 16, boxes % 16
    rise = (sub // 2 - my_sub // 2) % 8
    far_core = (sub % 2 != my_sub % 2).astype(jnp.int32)
    return far_core * 256 + rise * 32 + (sub // 16) * 16 + slot


def body(
    fine_fields,
    fine_octant,
    mid_octant,
    shift_fine,
    shift_mid,
    interp_theta_mid,
    interp_phi_mid,
    interp_theta_top,
    interp_phi_top,
    partners,
    translation,
):
    my_sub = lax.axis_index("sub")
    fine = fine_fields.reshape(64, 2, 8, 128).transpose(0, 2, 1, 3).reshape(64, 16, 128)
    operator = translation.reshape(512, 2, 8, 128).transpose(0, 2, 1, 3).reshape(512, 16, 128)
    tables_of = (
        shift_fine.reshape(8, 32, 128).transpose(1, 0, 2).reshape(256, 128),
        shift_mid.reshape(8, 128, 128).transpose(1, 0, 2).reshape(1024, 128),
        interp_theta_mid.T,
        interp_phi_mid.T,
        interp_theta_top.T,
        interp_phi_top.T,
    )
    slots = slot_of(partners, my_sub)
    top = call_up(fine, fine_octant, mid_octant, tables_of)
    prepared = call_prepare(tables_of)
    pairs = [
        [(x * 16 + i) * 16 + d for x in range(2) for d in range(16)] for i in range(16)
    ]
    own = lax.all_to_all(
        top, ("sub", "dir"), split_axis=0, concat_axis=0, tiled=True, axis_index_groups=pairs
    )
    near, far = gather_tops(own)
    partial = call_near(slots, operator, near)
    incoming = call_far(slots, operator, far, partial)
    parent = lax.all_to_all(incoming, "dir", split_axis=0, concat_axis=0, tiled=True)
    result = call_down(parent, fine_octant, mid_octant, prepared)
    return result.reshape(64, 8, 2, 128).transpose(0, 2, 1, 3).reshape(64, 2, 1024)


def solution(mesh):
    in_specs = (
        P(("sub", "dir"), None, None),
        P(("sub", "dir")),
        P("sub"),
        P(),
        P(),
        P(),
        P(),
        P(),
        P(),
        P("sub", None),
        P("sub", None, None, "dir"),
    )
    out_specs = P(("sub", "dir"), None, None)
    return jax.shard_map(body, mesh=mesh, in_specs=in_specs, out_specs=out_specs, check_vma=False)
```

```python
import jax
import jax.numpy as jnp
from jax import lax
from jax.experimental import pallas as pl
from jax.experimental.pallas import tpu as pltpu
from jax.sharding import PartitionSpec as P

F32 = jnp.float32
BF16 = jnp.bfloat16
VMEM = pl.BlockSpec(memory_space=pltpu.VMEM)
SMEM = pl.BlockSpec(memory_space=pltpu.SMEM)
UP_GROUP, TOP_GROUP, DOWN_GROUP = 4, 2, 4
ANY = pl.BlockSpec(memory_space=pl.ANY)


def split(x):
    high = x.astype(BF16)
    return high, (x - high.astype(F32)).astype(BF16)


def dot(a, b, dims=((1,), (0,))):
    return lax.dot_general(a, b, (dims, ((), ())), preferred_element_type=F32)


def onehot(shape, source):
    rows = lax.broadcasted_iota(jnp.int32, shape, 0)
    cols = lax.broadcasted_iota(jnp.int32, shape, 1)
    return jnp.where(source(rows, cols), 1.0, 0.0).astype(BF16)


def cos_sin(angles):
    half = angles * 0.5
    square = half * half
    sine = -1.0 / 39916800.0
    for term in (1.0 / 362880.0, -1.0 / 5040.0, 1.0 / 120.0, -1.0 / 6.0, 1.0):
        sine = sine * square + term
    sine = sine * half
    cosine = 1.0 / 479001600.0
    for term in (-1.0 / 3628800.0, 1.0 / 40320.0, -1.0 / 720.0, 1.0 / 24.0, -0.5, 1.0):
        cosine = cosine * square + term
    return 1.0 - 2.0 * (sine * sine), 2.0 * (sine * cosine)


def group_transpose(v):
    lane = lax.broadcasted_iota(jnp.int32, v[0].shape, 1)
    low = lane < 64
    even = (lane // 32) % 2 == 0
    roll = lambda x, by: pltpu.roll(x, by, 1)
    x0 = jnp.where(low, v[0], roll(v[2], 64))
    x2 = jnp.where(low, roll(v[0], 64), v[2])
    x1 = jnp.where(low, v[1], roll(v[3], 64))
    x3 = jnp.where(low, roll(v[1], 64), v[3])
    return [
        jnp.where(even, x0, roll(x1, 32)),
        jnp.where(even, roll(x0, 96), x1),
        jnp.where(even, x2, roll(x3, 32)),
        jnp.where(even, roll(x2, 96), x3),
    ]


def invert(octants, inverse, count, first):
    def step(i, _):
        inverse[(i // 8) * 8 + octants[first + i]] = i
        return 0

    lax.fori_loop(0, count, step, 0, unroll=8)


def fine_tables(angle_ref, cos_ref, sin_ref):
    for pair in range(4):
        first = angle_ref[pl.ds(2 * pair, 32, stride=8), :]
        second = angle_ref[pl.ds(2 * pair + 1, 32, stride=8), :]
        low = lax.broadcasted_iota(jnp.int32, first.shape, 1) < 64
        for odd, angles in enumerate(
            (
                jnp.where(low, first, pltpu.roll(second, 64, 1)),
                jnp.where(low, pltpu.roll(first, 64, 1), second),
            )
        ):
            cosine, sine = cos_sin(angles)
            cos_ref[pair, pl.ds(32 * odd, 32), :] = cosine
            sin_ref[pair, pl.ds(32 * odd, 32), :] = sine


def top_tables(angle_ref, cos_ref, sin_ref):
    for i in range(16):
        cosine, sine = cos_sin(angle_ref[pl.ds(64 * i, 64), :])
        cos_ref[pl.ds(64 * i, 64), :] = cosine
        sin_ref[pl.ds(64 * i, 64), :] = sine


def block_diagonal(matrix, copies):
    n, k = matrix.shape
    spread = onehot((k, copies * k), lambda r, c: c % k == r)
    out = []
    for part in split(matrix):
        wide = dot(part, spread)
        tall = jnp.concatenate([wide] * copies, axis=0)
        rows = lax.broadcasted_iota(jnp.int32, tall.shape, 0) // n
        cols = lax.broadcasted_iota(jnp.int32, tall.shape, 1) // k
        out.append(jnp.where(rows == cols, tall, 0.0).astype(BF16))
    return out


def theta_up(theta, rows, cols):
    targets, sources = theta.shape[1], theta.shape[0]
    high, low = [
        dot(onehot((targets, targets), rows), part, ((1,), (1,))).astype(BF16)
        for part in split(theta)
    ]
    wide = (sources, 3 * sources)
    order = lambda r, c: cols(r, c % sources)
    first = onehot(wide, lambda r, c: order(r, c) & (c < 2 * sources))
    last = onehot(wide, lambda r, c: order(r, c) & (c >= 2 * sources))
    return (dot(high, first) + dot(low, last)).astype(BF16)


def theta_down(theta, rows, cols):
    sources, targets = theta.shape
    high, low = [
        dot(onehot((sources, sources), rows), part).astype(BF16) for part in split(theta)
    ]
    wide = (targets, 3 * targets)
    order = lambda r, c: cols(r, c % targets)
    first = onehot(wide, lambda r, c: order(r, c) & (c < 2 * targets))
    last = onehot(wide, lambda r, c: order(r, c) & (c >= 2 * targets))
    return (dot(high, first) + dot(low, last)).astype(BF16)


def up_kernel(
    fine, fine_oct, mid_oct, angle_fine, angle_mid, theta_mid, phi_mid, theta_top, phi_top,
    out, fine_inv, mid_inv, cos_f, sin_f, cos_t, sin_t, mids,
):
    invert(fine_oct, fine_inv, 64, 0)
    invert(mid_oct, mid_inv, 8, lax.axis_index("dir") * 8)
    fine_tables(angle_fine, cos_f, sin_f)
    top_tables(angle_mid, cos_t, sin_t)
    a_mid = theta_up(
        theta_mid[...],
        lambda r, c: c == 2 * (r % 32) + r // 32,
        lambda r, c: r == 4 * (c % 8) + c // 8,
    )
    a_top = theta_up(
        theta_top[...], lambda r, c: r == c, lambda r, c: r == 2 * (c % 32) + c // 32
    )
    b_high, b_low = block_diagonal(phi_mid[...], 4)
    b_mid = jnp.concatenate([b_high, b_high, b_low], axis=0)
    b_high, b_low = block_diagonal(phi_top[...], 2)
    b_top = jnp.concatenate([b_high, b_high, b_low], axis=0)
    for first in range(0, 8, UP_GROUP):
        chunks = []
        for octant in range(first, first + UP_GROUP):
            m = mid_inv[octant]
            for h in range(2):
                boxes = [fine_inv[m * 8 + 4 * h + b] for b in range(4)]
                for c in range(2):
                    v = [fine[box, pl.ds(c, 8, stride=2), :] for box in boxes]
                    chunks.append(jnp.concatenate(group_transpose(v), axis=0))
        w_high, w_low = split(jnp.concatenate(chunks, axis=1))
        y = dot(a_mid, jnp.concatenate([w_high, w_low, w_high], axis=0))
        y = jnp.concatenate([y[:, 128 * i : 128 * i + 128] for i in range(len(chunks))], axis=0)
        y_high, y_low = split(y)
        z = dot(jnp.concatenate([y_high, y_low, y_high], axis=1), b_mid)
        for g in range(UP_GROUP):
            real, imag = 0.0, 0.0
            for h in range(2):
                row = 256 * g + 128 * h
                for j in range(2):
                    re = z[row : row + 64, 128 * j : 128 * j + 128]
                    im = z[row + 64 : row + 128, 128 * j : 128 * j + 128]
                    cosine, sine = cos_f[2 * h + j], sin_f[2 * h + j]
                    real = real + (re * cosine - im * sine)
                    imag = imag + (re * sine + im * cosine)
            mids[first + g, 0] = real + pltpu.roll(real, 64, 1)
            mids[first + g, 1] = imag + pltpu.roll(imag, 64, 1)
    low = lax.broadcasted_iota(jnp.int32, (64, 128), 1) < 64
    top = [0.0, 0.0]
    for first in range(0, 4, TOP_GROUP):
        chunks = [
            jnp.where(low, mids[2 * pair, c], mids[2 * pair + 1, c])
            for pair in range(first, first + TOP_GROUP)
            for c in range(2)
        ]
        w_high, w_low = split(jnp.concatenate(chunks, axis=1))
        y = dot(a_top, jnp.concatenate([w_high, w_low, w_high], axis=0))
        y = jnp.concatenate([y[:, 128 * i : 128 * i + 128] for i in range(len(chunks))], axis=0)
        y_high, y_low = split(y)
        z = dot(jnp.concatenate([y_high, y_low, y_high], axis=1), b_top)
        for g in range(TOP_GROUP):
            for j in range(2):
                re = z[256 * g : 256 * g + 128, 128 * j : 128 * j + 128]
                im = z[256 * g + 128 : 256 * g + 256, 128 * j : 128 * j + 128]
                octant = 2 * (first + g) + j
                cosine = cos_t[pl.ds(octant, 128, stride=8), :]
                sine = sin_t[pl.ds(octant, 128, stride=8), :]
                top[0] = top[0] + (re * cosine - im * sine)
                top[1] = top[1] + (re * sine + im * cosine)
    for c in range(2):
        for d in range(16):
            for x in range(2):
                out[16 * x + d, pl.ds(8 * c, 8), :] = top[c][8 * d : 8 * d + 8]


def prepare_kernel(
    angle_fine, angle_mid, theta_mid, phi_mid, theta_top, phi_top,
    cos_f, sin_f, cos_t, sin_t, a_mid, b_mid, a_top, b_top,
):
    fine_tables(angle_fine, cos_f, sin_f)
    top_tables(angle_mid, cos_t, sin_t)
    b_high, b_low = [jnp.concatenate([part, part], axis=0) for part in split(phi_top[...])]
    b_top[...] = jnp.concatenate([b_high, b_high, b_low], axis=1)
    a_top[...] = theta_down(
        theta_top[...], lambda r, c: c == 2 * (r % 32) + r // 32, lambda r, c: r == c
    )
    b_high, b_low = block_diagonal(phi_mid[...], 4)
    b_mid[...] = jnp.concatenate([b_high, b_high, b_low], axis=1)
    a_mid[...] = theta_down(
        theta_mid[...],
        lambda r, c: c == 4 * (r % 8) + r // 8,
        lambda r, c: r == 2 * (c % 32) + c // 32,
    )


def down_kernel(
    parent, fine_oct, mid_oct, cos_f, sin_f, cos_t, sin_t, a_mid, b_mid, a_top, b_top,
    out, fine_inv, mid_inv,
):
    invert(fine_oct, fine_inv, 64, 0)
    invert(mid_oct, mid_inv, 8, lax.axis_index("dir") * 8)
    field = [
        jnp.concatenate([parent[d, pl.ds(8 * c, 8), :] for d in range(16)], axis=0)
        for c in range(2)
    ]
    across = ((1,), (1,))
    for first in range(0, 8, DOWN_GROUP):
        rows = []
        for octant in range(first, first + DOWN_GROUP):
            cosine = cos_t[pl.ds(octant, 128, stride=8), :]
            sine = sin_t[pl.ds(octant, 128, stride=8), :]
            rows.append(field[0] * cosine + field[1] * sine)
            rows.append(field[1] * cosine - field[0] * sine)
        x_high, x_low = split(jnp.concatenate(rows, axis=0))
        y = dot(jnp.concatenate([x_high, x_low, x_high], axis=1), b_top[...], across)
        y = jnp.concatenate([y[128 * i : 128 * i + 128] for i in range(len(rows))], axis=1)
        y_high, y_low = split(y)
        mid = dot(a_top[...], jnp.concatenate([y_high, y_low, y_high], axis=0))
        rows = []
        for g in range(DOWN_GROUP):
            re, im = mid[:, 256 * g : 256 * g + 128], mid[:, 256 * g + 128 : 256 * g + 256]
            for h in range(2):
                c0, s0 = cos_f[2 * h], sin_f[2 * h]
                c1, s1 = cos_f[2 * h + 1], sin_f[2 * h + 1]
                rows.append(jnp.concatenate([re * c0 + im * s0, re * c1 + im * s1], axis=1))
                rows.append(jnp.concatenate([im * c0 - re * s0, im * c1 - re * s1], axis=1))
        x_high, x_low = split(jnp.concatenate(rows, axis=0))
        y = dot(jnp.concatenate([x_high, x_low, x_high], axis=1), b_mid[...], across)
        y = jnp.concatenate([y[64 * i : 64 * i + 64] for i in range(len(rows))], axis=1)
        y_high, y_low = split(y)
        w = dot(a_mid[...], jnp.concatenate([y_high, y_low, y_high], axis=0))
        for g in range(DOWN_GROUP):
            m = mid_inv[first + g]
            for h in range(2):
                boxes = [fine_inv[m * 8 + 4 * h + b] for b in range(4)]
                for c in range(2):
                    lanes = 128 * (4 * g + 2 * h + c)
                    v = group_transpose(
                        [w[8 * i : 8 * i + 8, lanes : lanes + 128] for i in range(4)]
                    )
                    for b in range(4):
                        out[boxes[b], pl.ds(c, 8, stride=2), :] = v[b]


def in_vmem(x):
    return pltpu.with_memory_space_constraint(x, pltpu.VMEM)


INVERSES = [pltpu.SMEM((64,), jnp.int32), pltpu.SMEM((8,), jnp.int32)]
TABLES = [((4, 64, 128), F32)] * 2 + [((1024, 128), F32)] * 2
DOWN_MATRICES = [((32, 192), BF16), ((128, 768), BF16), ((64, 384), BF16), ((128, 384), BF16)]


def call_up(fine, fine_oct, mid_oct, tables_of):
    return pl.pallas_call(
        up_kernel,
        out_shape=pltpu.VMEM((32, 16, 128), F32),
        in_specs=[VMEM, SMEM, SMEM] + [VMEM] * 6,
        out_specs=VMEM,
        scratch_shapes=INVERSES
        + [pltpu.VMEM(*table) for table in TABLES]
        + [pltpu.VMEM((8, 2, 64, 128), F32)],
        name="upward",
    )(fine, fine_oct, mid_oct, *tables_of)


def call_prepare(tables_of):
    shapes = TABLES + DOWN_MATRICES
    return pl.pallas_call(
        prepare_kernel,
        out_shape=[pltpu.VMEM(*shape) for shape in shapes],
        in_specs=[VMEM] * 6,
        out_specs=[VMEM] * len(shapes),
        cost_estimate=pl.CostEstimate(flops=200000000, bytes_accessed=2000000, transcendentals=0),
        compiler_params=pltpu.CompilerParams(vmem_limit_bytes=12 * 2**20),
        name="prepare",
    )(*tables_of)


def call_down(parent, fine_oct, mid_oct, prepared):
    return pl.pallas_call(
        down_kernel,
        out_shape=jax.ShapeDtypeStruct((64, 16, 128), F32),
        in_specs=[VMEM, SMEM, SMEM] + [VMEM] * 8,
        out_specs=VMEM,
        scratch_shapes=INVERSES,
        compiler_params=pltpu.CompilerParams(vmem_limit_bytes=24 * 2**20),
        name="downward",
    )(in_vmem(parent), fine_oct, mid_oct, *[in_vmem(x) for x in prepared])


def add_pairs(slots, tables, fields, t, total):
    real, imag = [total[0]] + [0.0] * 3, [total[1]] + [0.0] * 3
    for k in range(32):
        n = slots[t, k]
        fr, fi = fields[n, pl.ds(0, 8), :], fields[n, pl.ds(8, 8), :]
        tr = tables[32 * t + k, pl.ds(0, 8, stride=2), :]
        ti = tables[32 * t + k, pl.ds(1, 8, stride=2), :]
        real[k % 4] = real[k % 4] + (fr * tr - fi * ti)
        imag[k % 4] = imag[k % 4] + (fr * ti + fi * tr)
    return (real[0] + real[1]) + (real[2] + real[3]), (imag[0] + imag[1]) + (imag[2] + imag[3])


def near_kernel(slots, tables, near, out):
    for t in range(16):
        real, imag = add_pairs(slots, tables, near, t, (0.0, 0.0))
        out[t, pl.ds(0, 8), :] = real
        out[t, pl.ds(8, 8), :] = imag


def far_kernel(slots, tables, far, partial, out):
    for t in range(16):
        total = partial[t, pl.ds(0, 8), :], partial[t, pl.ds(8, 8), :]
        real, imag = add_pairs(slots, tables, far, t, total)
        out[t, pl.ds(0, 8), :] = real
        out[t, pl.ds(8, 8), :] = imag


def call_near(slots, tables, near):
    return pl.pallas_call(
        near_kernel,
        out_shape=pltpu.VMEM((16, 16, 128), F32),
        in_specs=[SMEM, VMEM, VMEM],
        out_specs=VMEM,
        cost_estimate=pl.CostEstimate(flops=200000000, bytes_accessed=6000000, transcendentals=0),
        compiler_params=pltpu.CompilerParams(vmem_limit_bytes=6 * 2**20),
        name="near",
    )(slots, in_vmem(tables), in_vmem(near))


def call_far(slots, tables, far, partial):
    return pl.pallas_call(
        far_kernel,
        out_shape=pltpu.VMEM((16, 16, 128), F32),
        in_specs=[SMEM, VMEM, VMEM, VMEM],
        out_specs=VMEM,
        compiler_params=pltpu.CompilerParams(vmem_limit_bytes=6 * 2**20),
        name="far",
    )(slots, in_vmem(tables), in_vmem(far), in_vmem(partial))


def permutations():
    place = lambda x, y, core: x * 16 + (y % 8) * 2 + core
    every = [(x, y, core) for x in range(2) for y in range(8) for core in range(2)]
    ring = lambda by: [(place(x, y, c), place(x, y + (by, -by)[c], 1 - c)) for x, y, c in every]
    other = [(place(x, y, c), place(x, y, 1 - c)) for x, y, c in every]
    return ring(1), ring(-1), other


def gather_tops(own):
    first, second, other = permutations()
    send = lambda x, perm: lax.ppermute(x, "sub", perm)
    up, down = [], []
    a = b = own
    for _ in range(3):
        a, b = send(b, first), send(a, second)
        up.append(a)
        down.append(b)
    half = own.shape[0] // 2
    fourth = [send(b[:half], first), send(a[half:], second)]
    mine = [own] + up + fourth + down[::-1]
    near = jnp.concatenate(mine + [jnp.zeros_like(own[:1])], axis=0)
    return near, send(near, other)


def slot_of(boxes, my_sub):
    sub, slot = boxes // 16, boxes % 16
    rise = (sub // 2 - my_sub // 2) % 8
    holder = (sub + rise) % 2
    step = jnp.where(holder == 0, rise, (8 - rise) % 8)
    far = (holder != my_sub % 2).astype(jnp.int32)
    return far * 256 + step * 32 + (sub // 16) * 16 + slot


def body(
    fine_fields,
    fine_octant,
    mid_octant,
    shift_fine,
    shift_mid,
    interp_theta_mid,
    interp_phi_mid,
    interp_theta_top,
    interp_phi_top,
    partners,
    translation,
):
    my_sub = lax.axis_index("sub")
    fine = fine_fields.reshape(64, 2, 8, 128).transpose(0, 2, 1, 3).reshape(64, 16, 128)
    operator = translation.reshape(512, 2, 8, 128).transpose(0, 2, 1, 3).reshape(512, 16, 128)
    tables_of = (
        shift_fine.reshape(8, 32, 128).transpose(1, 0, 2).reshape(256, 128),
        shift_mid.reshape(8, 128, 128).transpose(1, 0, 2).reshape(1024, 128),
        interp_theta_mid.T,
        interp_phi_mid.T,
        interp_theta_top.T,
        interp_phi_top.T,
    )
    slots = slot_of(partners, my_sub)
    near_slots = jnp.minimum(slots, 256)
    far_slots = jnp.where(slots < 256, 256, slots - 256)
    top = call_up(fine, fine_octant, mid_octant, tables_of)
    prepared = call_prepare(tables_of)
    pairs = [
        [(x * 16 + i) * 16 + d for x in range(2) for d in range(16)] for i in range(16)
    ]
    own = lax.all_to_all(
        top, ("sub", "dir"), split_axis=0, concat_axis=0, tiled=True, axis_index_groups=pairs
    )
    near, far = gather_tops(own)
    partial = call_near(near_slots, operator, near)
    incoming = call_far(far_slots, operator, far, partial)
    parent = lax.all_to_all(incoming, "dir", split_axis=0, concat_axis=0, tiled=True)
    result = call_down(parent, fine_octant, mid_octant, prepared)
    return result.reshape(64, 8, 2, 128).transpose(0, 2, 1, 3).reshape(64, 2, 1024)


def solution(mesh):
    in_specs = (
        P(("sub", "dir"), None, None),
        P(("sub", "dir")),
        P("sub"),
        P(),
        P(),
        P(),
        P(),
        P(),
        P(),
        P("sub", None),
        P("sub", None, None, "dir"),
    )
    out_specs = P(("sub", "dir"), None, None)
    return jax.shard_map(body, mesh=mesh, in_specs=in_specs, out_specs=out_specs, check_vma=False)
```

```python
import jax
import jax.numpy as jnp
from jax import lax
from jax.experimental import pallas as pl
from jax.experimental.pallas import tpu as pltpu
from jax.sharding import PartitionSpec as P


F32 = jnp.float32
BF16 = jnp.bfloat16
VMEM = pl.BlockSpec(memory_space=pltpu.VMEM)
SMEM = pl.BlockSpec(memory_space=pltpu.SMEM)
UP_GROUP, TOP_GROUP, DOWN_GROUP = 4, 2, 4
ANY = pl.BlockSpec(memory_space=pl.ANY)


def split(x):
    high = x.astype(BF16)
    return high, (x - high.astype(F32)).astype(BF16)


def dot(a, b, dims=((1,), (0,))):
    return lax.dot_general(a, b, (dims, ((), ())), preferred_element_type=F32)


def onehot(shape, source):
    rows = lax.broadcasted_iota(jnp.int32, shape, 0)
    cols = lax.broadcasted_iota(jnp.int32, shape, 1)
    return jnp.where(source(rows, cols), 1.0, 0.0).astype(BF16)


def cos_sin(angles):
    half = angles * 0.5
    square = half * half
    sine = -1.0 / 39916800.0
    for term in (1.0 / 362880.0, -1.0 / 5040.0, 1.0 / 120.0, -1.0 / 6.0, 1.0):
        sine = sine * square + term
    sine = sine * half
    cosine = 1.0 / 479001600.0
    for term in (-1.0 / 3628800.0, 1.0 / 40320.0, -1.0 / 720.0, 1.0 / 24.0, -0.5, 1.0):
        cosine = cosine * square + term
    return 1.0 - 2.0 * (sine * sine), 2.0 * (sine * cosine)


def group_transpose(v):
    lane = lax.broadcasted_iota(jnp.int32, v[0].shape, 1)
    low = lane < 64
    even = (lane // 32) % 2 == 0
    roll = lambda x, by: pltpu.roll(x, by, 1)
    x0 = jnp.where(low, v[0], roll(v[2], 64))
    x2 = jnp.where(low, roll(v[0], 64), v[2])
    x1 = jnp.where(low, v[1], roll(v[3], 64))
    x3 = jnp.where(low, roll(v[1], 64), v[3])
    return [
        jnp.where(even, x0, roll(x1, 32)),
        jnp.where(even, roll(x0, 96), x1),
        jnp.where(even, x2, roll(x3, 32)),
        jnp.where(even, roll(x2, 96), x3),
    ]


def invert(octants, inverse, count, first):
    def step(i, _):
        inverse[(i // 8) * 8 + octants[first + i]] = i
        return 0

    lax.fori_loop(0, count, step, 0, unroll=8)


def fine_tables(angle_ref, cos_ref, sin_ref):
    for pair in range(4):
        first = angle_ref[pl.ds(2 * pair, 32, stride=8), :]
        second = angle_ref[pl.ds(2 * pair + 1, 32, stride=8), :]
        low = lax.broadcasted_iota(jnp.int32, first.shape, 1) < 64
        for odd, angles in enumerate(
            (
                jnp.where(low, first, pltpu.roll(second, 64, 1)),
                jnp.where(low, pltpu.roll(first, 64, 1), second),
            )
        ):
            cosine, sine = cos_sin(angles)
            cos_ref[pair, pl.ds(32 * odd, 32), :] = cosine
            sin_ref[pair, pl.ds(32 * odd, 32), :] = sine


def top_tables(angle_ref, cos_ref, sin_ref):
    for i in range(16):
        cosine, sine = cos_sin(angle_ref[pl.ds(64 * i, 64), :])
        cos_ref[pl.ds(64 * i, 64), :] = cosine
        sin_ref[pl.ds(64 * i, 64), :] = sine


def block_diagonal(matrix, copies):
    n, k = matrix.shape
    spread = onehot((k, copies * k), lambda r, c: c % k == r)
    out = []
    for part in split(matrix):
        wide = dot(part, spread)
        tall = jnp.concatenate([wide] * copies, axis=0)
        rows = lax.broadcasted_iota(jnp.int32, tall.shape, 0) // n
        cols = lax.broadcasted_iota(jnp.int32, tall.shape, 1) // k
        out.append(jnp.where(rows == cols, tall, 0.0).astype(BF16))
    return out


def theta_up(theta, rows, cols):
    targets, sources = theta.shape[1], theta.shape[0]
    high, low = [
        dot(onehot((targets, targets), rows), part, ((1,), (1,))).astype(BF16)
        for part in split(theta)
    ]
    wide = (sources, 3 * sources)
    order = lambda r, c: cols(r, c % sources)
    first = onehot(wide, lambda r, c: order(r, c) & (c < 2 * sources))
    last = onehot(wide, lambda r, c: order(r, c) & (c >= 2 * sources))
    return (dot(high, first) + dot(low, last)).astype(BF16)


def theta_down(theta, rows, cols):
    sources, targets = theta.shape
    high, low = [
        dot(onehot((sources, sources), rows), part).astype(BF16) for part in split(theta)
    ]
    wide = (targets, 3 * targets)
    order = lambda r, c: cols(r, c % targets)
    first = onehot(wide, lambda r, c: order(r, c) & (c < 2 * targets))
    last = onehot(wide, lambda r, c: order(r, c) & (c >= 2 * targets))
    return (dot(high, first) + dot(low, last)).astype(BF16)


def up_kernel(
    fine_hbm, fine_oct, mid_oct, angle_fine_hbm, angle_mid_hbm,
    theta_mid, phi_mid, theta_top, phi_top,
    out, fine_inv, mid_inv, cos_f, sin_f, cos_t, sin_t, mids,
    fine, angle_fine, angle_mid, sems,
):
    loads = [
        pltpu.make_async_copy(source, target, sems.at[i])
        for i, (source, target) in enumerate(
            ((angle_fine_hbm, angle_fine), (fine_hbm, fine), (angle_mid_hbm, angle_mid))
        )
    ]
    for load in loads:
        load.start()
    invert(fine_oct, fine_inv, 64, 0)
    invert(mid_oct, mid_inv, 8, lax.axis_index("dir") * 8)
    a_mid = theta_up(
        theta_mid[...],
        lambda r, c: c == 2 * (r % 32) + r // 32,
        lambda r, c: r == 4 * (c % 8) + c // 8,
    )
    a_top = theta_up(
        theta_top[...], lambda r, c: r == c, lambda r, c: r == 2 * (c % 32) + c // 32
    )
    b_high, b_low = block_diagonal(phi_mid[...], 4)
    b_mid = jnp.concatenate([b_high, b_high, b_low], axis=0)
    b_high, b_low = block_diagonal(phi_top[...], 2)
    b_top = jnp.concatenate([b_high, b_high, b_low], axis=0)
    loads[0].wait()
    fine_tables(angle_fine, cos_f, sin_f)
    loads[1].wait()
    for first in range(0, 8, UP_GROUP):
        chunks = []
        for octant in range(first, first + UP_GROUP):
            m = mid_inv[octant]
            for h in range(2):
                boxes = [fine_inv[m * 8 + 4 * h + b] for b in range(4)]
                for c in range(2):
                    v = [fine[box, pl.ds(c, 8, stride=2), :] for box in boxes]
                    chunks.append(jnp.concatenate(group_transpose(v), axis=0))
        w_high, w_low = split(jnp.concatenate(chunks, axis=1))
        y = dot(a_mid, jnp.concatenate([w_high, w_low, w_high], axis=0))
        y = jnp.concatenate([y[:, 128 * i : 128 * i + 128] for i in range(len(chunks))], axis=0)
        y_high, y_low = split(y)
        z = dot(jnp.concatenate([y_high, y_low, y_high], axis=1), b_mid)
        for g in range(UP_GROUP):
            real, imag = 0.0, 0.0
            for h in range(2):
                row = 256 * g + 128 * h
                for j in range(2):
                    re = z[row : row + 64, 128 * j : 128 * j + 128]
                    im = z[row + 64 : row + 128, 128 * j : 128 * j + 128]
                    cosine, sine = cos_f[2 * h + j], sin_f[2 * h + j]
                    real = real + (re * cosine - im * sine)
                    imag = imag + (re * sine + im * cosine)
            mids[first + g, 0] = real + pltpu.roll(real, 64, 1)
            mids[first + g, 1] = imag + pltpu.roll(imag, 64, 1)
    loads[2].wait()
    top_tables(angle_mid, cos_t, sin_t)
    low = lax.broadcasted_iota(jnp.int32, (64, 128), 1) < 64
    top = [0.0, 0.0]
    for first in range(0, 4, TOP_GROUP):
        chunks = [
            jnp.where(low, mids[2 * pair, c], mids[2 * pair + 1, c])
            for pair in range(first, first + TOP_GROUP)
            for c in range(2)
        ]
        w_high, w_low = split(jnp.concatenate(chunks, axis=1))
        y = dot(a_top, jnp.concatenate([w_high, w_low, w_high], axis=0))
        y = jnp.concatenate([y[:, 128 * i : 128 * i + 128] for i in range(len(chunks))], axis=0)
        y_high, y_low = split(y)
        z = dot(jnp.concatenate([y_high, y_low, y_high], axis=1), b_top)
        for g in range(TOP_GROUP):
            for j in range(2):
                re = z[256 * g : 256 * g + 128, 128 * j : 128 * j + 128]
                im = z[256 * g + 128 : 256 * g + 256, 128 * j : 128 * j + 128]
                octant = 2 * (first + g) + j
                cosine = cos_t[pl.ds(octant, 128, stride=8), :]
                sine = sin_t[pl.ds(octant, 128, stride=8), :]
                top[0] = top[0] + (re * cosine - im * sine)
                top[1] = top[1] + (re * sine + im * cosine)
    for c in range(2):
        for d in range(16):
            for x in range(2):
                out[16 * x + d, pl.ds(8 * c, 8), :] = top[c][8 * d : 8 * d + 8]


def prepare_kernel(
    angle_fine, angle_mid, theta_mid, phi_mid, theta_top, phi_top,
    cos_f, sin_f, cos_t, sin_t, a_mid, b_mid, a_top, b_top,
):
    fine_tables(angle_fine, cos_f, sin_f)
    top_tables(angle_mid, cos_t, sin_t)
    b_high, b_low = [jnp.concatenate([part, part], axis=0) for part in split(phi_top[...])]
    b_top[...] = jnp.concatenate([b_high, b_high, b_low], axis=1)
    a_top[...] = theta_down(
        theta_top[...], lambda r, c: c == 2 * (r % 32) + r // 32, lambda r, c: r == c
    )
    b_high, b_low = block_diagonal(phi_mid[...], 4)
    b_mid[...] = jnp.concatenate([b_high, b_high, b_low], axis=1)
    a_mid[...] = theta_down(
        theta_mid[...],
        lambda r, c: c == 4 * (r % 8) + r // 8,
        lambda r, c: r == 2 * (c % 32) + c // 32,
    )


def down_kernel(
    parent, fine_oct, mid_oct, cos_f, sin_f, cos_t, sin_t, a_mid, b_mid, a_top, b_top,
    out, fine_inv, mid_inv,
):
    invert(fine_oct, fine_inv, 64, 0)
    invert(mid_oct, mid_inv, 8, lax.axis_index("dir") * 8)
    field = [
        jnp.concatenate([parent[d, pl.ds(8 * c, 8), :] for d in range(16)], axis=0)
        for c in range(2)
    ]
    across = ((1,), (1,))
    for first in range(0, 8, DOWN_GROUP):
        rows = []
        for octant in range(first, first + DOWN_GROUP):
            cosine = cos_t[pl.ds(octant, 128, stride=8), :]
            sine = sin_t[pl.ds(octant, 128, stride=8), :]
            rows.append(field[0] * cosine + field[1] * sine)
            rows.append(field[1] * cosine - field[0] * sine)
        x_high, x_low = split(jnp.concatenate(rows, axis=0))
        y = dot(jnp.concatenate([x_high, x_low, x_high], axis=1), b_top[...], across)
        y = jnp.concatenate([y[128 * i : 128 * i + 128] for i in range(len(rows))], axis=1)
        y_high, y_low = split(y)
        mid = dot(a_top[...], jnp.concatenate([y_high, y_low, y_high], axis=0))
        rows = []
        for g in range(DOWN_GROUP):
            re, im = mid[:, 256 * g : 256 * g + 128], mid[:, 256 * g + 128 : 256 * g + 256]
            for h in range(2):
                c0, s0 = cos_f[2 * h], sin_f[2 * h]
                c1, s1 = cos_f[2 * h + 1], sin_f[2 * h + 1]
                rows.append(jnp.concatenate([re * c0 + im * s0, re * c1 + im * s1], axis=1))
                rows.append(jnp.concatenate([im * c0 - re * s0, im * c1 - re * s1], axis=1))
        x_high, x_low = split(jnp.concatenate(rows, axis=0))
        y = dot(jnp.concatenate([x_high, x_low, x_high], axis=1), b_mid[...], across)
        y = jnp.concatenate([y[64 * i : 64 * i + 64] for i in range(len(rows))], axis=1)
        y_high, y_low = split(y)
        w = dot(a_mid[...], jnp.concatenate([y_high, y_low, y_high], axis=0))
        for g in range(DOWN_GROUP):
            m = mid_inv[first + g]
            for h in range(2):
                boxes = [fine_inv[m * 8 + 4 * h + b] for b in range(4)]
                for c in range(2):
                    lanes = 128 * (4 * g + 2 * h + c)
                    v = group_transpose(
                        [w[8 * i : 8 * i + 8, lanes : lanes + 128] for i in range(4)]
                    )
                    for b in range(4):
                        out[boxes[b], pl.ds(c, 8, stride=2), :] = v[b]


def in_vmem(x):
    return pltpu.with_memory_space_constraint(x, pltpu.VMEM)


INVERSES = [pltpu.SMEM((64,), jnp.int32), pltpu.SMEM((8,), jnp.int32)]
TABLES = [((4, 64, 128), F32)] * 2 + [((1024, 128), F32)] * 2
DOWN_MATRICES = [((32, 192), BF16), ((128, 768), BF16), ((64, 384), BF16), ((128, 384), BF16)]


def call_up(fine, fine_oct, mid_oct, tables_of):
    return pl.pallas_call(
        up_kernel,
        out_shape=pltpu.VMEM((32, 16, 128), F32),
        in_specs=[ANY, SMEM, SMEM, ANY, ANY] + [VMEM] * 4,
        out_specs=VMEM,
        scratch_shapes=INVERSES
        + [pltpu.VMEM(*table) for table in TABLES]
        + [
            pltpu.VMEM((8, 2, 64, 128), F32),
            pltpu.VMEM((64, 16, 128), F32),
            pltpu.VMEM((256, 128), F32),
            pltpu.VMEM((1024, 128), F32),
            pltpu.SemaphoreType.DMA((3,)),
        ],
        name="upward",
    )(fine, fine_oct, mid_oct, *tables_of)


def call_prepare(tables_of):
    shapes = TABLES + DOWN_MATRICES
    return pl.pallas_call(
        prepare_kernel,
        out_shape=[pltpu.VMEM(*shape) for shape in shapes],
        in_specs=[VMEM] * 6,
        out_specs=[VMEM] * len(shapes),
        cost_estimate=pl.CostEstimate(flops=200000000, bytes_accessed=2000000, transcendentals=0),
        compiler_params=pltpu.CompilerParams(vmem_limit_bytes=12 * 2**20),
        name="prepare",
    )(*tables_of)


def call_down(parent, fine_oct, mid_oct, prepared):
    return pl.pallas_call(
        down_kernel,
        out_shape=jax.ShapeDtypeStruct((64, 16, 128), F32),
        in_specs=[VMEM, SMEM, SMEM] + [VMEM] * 8,
        out_specs=VMEM,
        scratch_shapes=INVERSES,
        compiler_params=pltpu.CompilerParams(vmem_limit_bytes=24 * 2**20),
        name="downward",
    )(in_vmem(parent), fine_oct, mid_oct, *[in_vmem(x) for x in prepared])


def add_pairs(slots, tables, fields, t, total):
    real, imag = [total[0]] + [0.0] * 3, [total[1]] + [0.0] * 3
    for k in range(32):
        fr, fi = [
            sum(field[slot[t, k], pl.ds(8 * c, 8), :] for slot, field in zip(slots, fields))
            for c in range(2)
        ]
        tr = tables[32 * t + k, pl.ds(0, 8, stride=2), :]
        ti = tables[32 * t + k, pl.ds(1, 8, stride=2), :]
        real[k % 4] = real[k % 4] + (fr * tr - fi * ti)
        imag[k % 4] = imag[k % 4] + (fr * ti + fi * tr)
    return (real[0] + real[1]) + (real[2] + real[3]), (imag[0] + imag[1]) + (imag[2] + imag[3])


def first_kernel(
    slots0, slots1, slots2, operator, fields0, fields1, fields2, tables, out, sems
):
    slots, fields = (slots0, slots1, slots2), (fields0, fields1, fields2)
    loads = [
        pltpu.make_async_copy(
            operator.at[pl.ds(32 * t, 32)], tables.at[pl.ds(32 * t, 32)], sems.at[t]
        )
        for t in range(16)
    ]
    for load in loads:
        load.start()
    for t in range(16):
        loads[t].wait()
        real, imag = add_pairs(slots, tables, fields, t, (0.0, 0.0))
        out[t, pl.ds(0, 8), :] = real
        out[t, pl.ds(8, 8), :] = imag


def last_kernel(slots, tables, fields, partial, out):
    for t in range(16):
        total = partial[t, pl.ds(0, 8), :], partial[t, pl.ds(8, 8), :]
        real, imag = add_pairs((slots,), tables, (fields,), t, total)
        out[t, pl.ds(0, 8), :] = real
        out[t, pl.ds(8, 8), :] = imag


def call_first(slots, operator, fields):
    return pl.pallas_call(
        first_kernel,
        out_shape=[pltpu.VMEM((512, 16, 128), F32), pltpu.VMEM((16, 16, 128), F32)],
        in_specs=[SMEM] * 3 + [pl.BlockSpec(memory_space=pltpu.HBM)] + [VMEM] * 3,
        out_specs=[VMEM, VMEM],
        scratch_shapes=[pltpu.SemaphoreType.DMA((16,))],
        cost_estimate=pl.CostEstimate(flops=200000000, bytes_accessed=6000000, transcendentals=0),
        compiler_params=pltpu.CompilerParams(vmem_limit_bytes=8 * 2**20),
        name="first",
    )(
        *slots,
        pltpu.with_memory_space_constraint(operator, pltpu.HBM),
        *[in_vmem(field) for field in fields],
    )


def call_last(slots, tables, fields, partial):
    return pl.pallas_call(
        last_kernel,
        out_shape=pltpu.VMEM((16, 16, 128), F32),
        in_specs=[SMEM, VMEM, VMEM, VMEM],
        out_specs=VMEM,
        compiler_params=pltpu.CompilerParams(vmem_limit_bytes=6 * 2**20),
        name="last",
    )(slots, in_vmem(tables), in_vmem(fields), in_vmem(partial))


def permutations():
    place = lambda x, y, core: x * 16 + (y % 8) * 2 + core
    every = [(x, y, core) for x in range(2) for y in range(8) for core in range(2)]
    ring = lambda by: [(place(x, y, c), place(x, y + (by, -by)[c], 1 - c)) for x, y, c in every]
    other = [(place(x, y, c), place(x, y, 1 - c)) for x, y, c in every]
    return ring(1), ring(-1), other


def gather_tops(own):
    first, second, other = permutations()
    send = lambda x, perm: lax.ppermute(x, "sub", perm)
    zero = jnp.zeros_like(own[:1])
    up, down = [], []
    a = b = own
    for _ in range(3):
        a, b = send(b, first), send(a, second)
        up.append(a)
        down.append(b)
    half = own.shape[0] // 2
    fourth_a = send(b[:half], first)
    fourth_b = send(a[half:], second)
    early = jnp.concatenate([own, up[0], up[1], down[1], down[0], zero], axis=0)
    early_far = send(early, other)
    late = jnp.concatenate([up[2], fourth_a, fourth_b, down[2], zero], axis=0)
    late_far = send(late, other)
    return early, late, early_far, late_far


def slots_of(boxes, my_sub):
    sub, slot = boxes // 16, boxes % 16
    rise = (sub // 2 - my_sub // 2) % 8
    holder = (sub + rise) % 2
    step = jnp.where(holder == 0, rise, (8 - rise) % 8)
    far = holder != my_sub % 2
    late = (step >= 3) & (step <= 5)
    place = jnp.where(step >= 3, step - 3, step) * 32 + (sub // 16) * 16 + slot
    early_slots = [jnp.where((far == side) & ~late, place, 160) for side in (False, True)]
    late_slots = [jnp.where((far == side) & late, place, 96) for side in (False, True)]
    return early_slots[0], late_slots[0], early_slots[1], late_slots[1]


def body(
    fine_fields,
    fine_octant,
    mid_octant,
    shift_fine,
    shift_mid,
    interp_theta_mid,
    interp_phi_mid,
    interp_theta_top,
    interp_phi_top,
    partners,
    translation,
):
    my_sub = lax.axis_index("sub")
    fine = fine_fields.reshape(64, 2, 8, 128).transpose(0, 2, 1, 3).reshape(64, 16, 128)
    operator = translation.reshape(512, 2, 8, 128).transpose(0, 2, 1, 3).reshape(512, 16, 128)
    tables_of = (
        shift_fine.reshape(8, 32, 128).transpose(1, 0, 2).reshape(256, 128),
        shift_mid.reshape(8, 128, 128).transpose(1, 0, 2).reshape(1024, 128),
        interp_theta_mid.T,
        interp_phi_mid.T,
        interp_theta_top.T,
        interp_phi_top.T,
    )
    slots = slots_of(partners, my_sub)
    top = call_up(fine, fine_octant, mid_octant, tables_of)
    prepared = call_prepare(tables_of)
    pairs = [
        [(x * 16 + i) * 16 + d for x in range(2) for d in range(16)] for i in range(16)
    ]
    own = lax.all_to_all(
        top, ("sub", "dir"), split_axis=0, concat_axis=0, tiled=True, axis_index_groups=pairs
    )
    fields = gather_tops(own)
    tables, partial = call_first(slots[:3], operator, fields[:3])
    incoming = call_last(slots[3], tables, fields[3], partial)
    parent = lax.all_to_all(incoming, "dir", split_axis=0, concat_axis=0, tiled=True)
    result = call_down(parent, fine_octant, mid_octant, prepared)
    return result.reshape(64, 8, 2, 128).transpose(0, 2, 1, 3).reshape(64, 2, 1024)


def solution(mesh):
    in_specs = (
        P(("sub", "dir"), None, None),
        P(("sub", "dir")),
        P("sub"),
        P(),
        P(),
        P(),
        P(),
        P(),
        P(),
        P("sub", None),
        P("sub", None, None, "dir"),
    )
    out_specs = P(("sub", "dir"), None, None)
    return jax.shard_map(body, mesh=mesh, in_specs=in_specs, out_specs=out_specs, check_vma=False)
```

```python
import jax
import jax.numpy as jnp
from jax import lax
from jax.experimental import pallas as pl
from jax.experimental.pallas import tpu as pltpu
from jax.sharding import PartitionSpec as P


F32 = jnp.float32
BF16 = jnp.bfloat16
VMEM = pl.BlockSpec(memory_space=pltpu.VMEM)
SMEM = pl.BlockSpec(memory_space=pltpu.SMEM)
UP_GROUP, TOP_GROUP, DOWN_GROUP = 4, 2, 4
ANY = pl.BlockSpec(memory_space=pl.ANY)


def split(x):
    high = x.astype(BF16)
    return high, (x - high.astype(F32)).astype(BF16)


def dot(a, b, dims=((1,), (0,))):
    return lax.dot_general(a, b, (dims, ((), ())), preferred_element_type=F32)


def onehot(shape, source):
    rows = lax.broadcasted_iota(jnp.int32, shape, 0)
    cols = lax.broadcasted_iota(jnp.int32, shape, 1)
    return jnp.where(source(rows, cols), 1.0, 0.0).astype(BF16)


def cos_sin(angles):
    half = angles * 0.5
    square = half * half
    sine = -1.0 / 39916800.0
    for term in (1.0 / 362880.0, -1.0 / 5040.0, 1.0 / 120.0, -1.0 / 6.0, 1.0):
        sine = sine * square + term
    sine = sine * half
    cosine = 1.0 / 479001600.0
    for term in (-1.0 / 3628800.0, 1.0 / 40320.0, -1.0 / 720.0, 1.0 / 24.0, -0.5, 1.0):
        cosine = cosine * square + term
    return 1.0 - 2.0 * (sine * sine), 2.0 * (sine * cosine)


def group_transpose(v):
    lane = lax.broadcasted_iota(jnp.int32, v[0].shape, 1)
    low = lane < 64
    even = (lane // 32) % 2 == 0
    roll = lambda x, by: pltpu.roll(x, by, 1)
    x0 = jnp.where(low, v[0], roll(v[2], 64))
    x2 = jnp.where(low, roll(v[0], 64), v[2])
    x1 = jnp.where(low, v[1], roll(v[3], 64))
    x3 = jnp.where(low, roll(v[1], 64), v[3])
    return [
        jnp.where(even, x0, roll(x1, 32)),
        jnp.where(even, roll(x0, 96), x1),
        jnp.where(even, x2, roll(x3, 32)),
        jnp.where(even, roll(x2, 96), x3),
    ]


def invert(octants, inverse, count, first):
    def step(i, _):
        inverse[(i // 8) * 8 + octants[first + i]] = i
        return 0

    lax.fori_loop(0, count, step, 0, unroll=8)


def fine_tables(angle_ref, cos_ref, sin_ref):
    for pair in range(4):
        first = angle_ref[pl.ds(2 * pair, 32, stride=8), :]
        second = angle_ref[pl.ds(2 * pair + 1, 32, stride=8), :]
        low = lax.broadcasted_iota(jnp.int32, first.shape, 1) < 64
        for odd, angles in enumerate(
            (
                jnp.where(low, first, pltpu.roll(second, 64, 1)),
                jnp.where(low, pltpu.roll(first, 64, 1), second),
            )
        ):
            cosine, sine = cos_sin(angles)
            cos_ref[pair, pl.ds(32 * odd, 32), :] = cosine
            sin_ref[pair, pl.ds(32 * odd, 32), :] = sine


def top_tables(angle_ref, cos_ref, sin_ref):
    for i in range(16):
        cosine, sine = cos_sin(angle_ref[pl.ds(64 * i, 64), :])
        cos_ref[pl.ds(64 * i, 64), :] = cosine
        sin_ref[pl.ds(64 * i, 64), :] = sine


def block_diagonal(matrix, copies):
    n, k = matrix.shape
    spread = onehot((k, copies * k), lambda r, c: c % k == r)
    out = []
    for part in split(matrix):
        wide = dot(part, spread)
        tall = jnp.concatenate([wide] * copies, axis=0)
        rows = lax.broadcasted_iota(jnp.int32, tall.shape, 0) // n
        cols = lax.broadcasted_iota(jnp.int32, tall.shape, 1) // k
        out.append(jnp.where(rows == cols, tall, 0.0).astype(BF16))
    return out


def theta_up(theta, rows, cols):
    targets, sources = theta.shape[1], theta.shape[0]
    high, low = [
        dot(onehot((targets, targets), rows), part, ((1,), (1,))).astype(BF16)
        for part in split(theta)
    ]
    wide = (sources, 3 * sources)
    order = lambda r, c: cols(r, c % sources)
    first = onehot(wide, lambda r, c: order(r, c) & (c < 2 * sources))
    last = onehot(wide, lambda r, c: order(r, c) & (c >= 2 * sources))
    return (dot(high, first) + dot(low, last)).astype(BF16)


def theta_down(theta, rows, cols):
    sources, targets = theta.shape
    high, low = [
        dot(onehot((sources, sources), rows), part).astype(BF16) for part in split(theta)
    ]
    wide = (targets, 3 * targets)
    order = lambda r, c: cols(r, c % targets)
    first = onehot(wide, lambda r, c: order(r, c) & (c < 2 * targets))
    last = onehot(wide, lambda r, c: order(r, c) & (c >= 2 * targets))
    return (dot(high, first) + dot(low, last)).astype(BF16)


def up_kernel(*refs):
    sources, (out, fine_inv, mid_inv, cos_f, sin_f, cos_t, sin_t, mids) = refs[:9], refs[9:17]
    targets, sems = refs[17:26], refs[26]
    loads = [
        pltpu.make_async_copy(source, target, sems.at[i])
        for i, (source, target) in enumerate(zip(sources, targets))
    ]
    fine, fine_oct, mid_oct, angle_fine, angle_mid, theta_mid, phi_mid, theta_top, phi_top = targets
    for i in (5, 6, 7, 8, 3, 1, 2, 0, 4):
        loads[i].start()
    for i in (5, 6, 7, 8):
        loads[i].wait()
    a_mid = theta_up(
        theta_mid[...],
        lambda r, c: c == 2 * (r % 32) + r // 32,
        lambda r, c: r == 4 * (c % 8) + c // 8,
    )
    a_top = theta_up(
        theta_top[...], lambda r, c: r == c, lambda r, c: r == 2 * (c % 32) + c // 32
    )
    b_high, b_low = block_diagonal(phi_mid[...], 4)
    b_mid = jnp.concatenate([b_high, b_high, b_low], axis=0)
    b_high, b_low = block_diagonal(phi_top[...], 2)
    b_top = jnp.concatenate([b_high, b_high, b_low], axis=0)
    loads[3].wait()
    fine_tables(angle_fine, cos_f, sin_f)
    loads[1].wait()
    loads[2].wait()
    invert(fine_oct, fine_inv, 64, 0)
    invert(mid_oct, mid_inv, 8, lax.axis_index("dir") * 8)
    loads[0].wait()
    for first in range(0, 8, UP_GROUP):
        chunks = []
        for octant in range(first, first + UP_GROUP):
            m = mid_inv[octant]
            for h in range(2):
                boxes = [fine_inv[m * 8 + 4 * h + b] for b in range(4)]
                for c in range(2):
                    v = [fine[box, pl.ds(c, 8, stride=2), :] for box in boxes]
                    chunks.append(jnp.concatenate(group_transpose(v), axis=0))
        w_high, w_low = split(jnp.concatenate(chunks, axis=1))
        y = dot(a_mid, jnp.concatenate([w_high, w_low, w_high], axis=0))
        y = jnp.concatenate([y[:, 128 * i : 128 * i + 128] for i in range(len(chunks))], axis=0)
        y_high, y_low = split(y)
        z = dot(jnp.concatenate([y_high, y_low, y_high], axis=1), b_mid)
        for g in range(UP_GROUP):
            real, imag = 0.0, 0.0
            for h in range(2):
                row = 256 * g + 128 * h
                for j in range(2):
                    re = z[row : row + 64, 128 * j : 128 * j + 128]
                    im = z[row + 64 : row + 128, 128 * j : 128 * j + 128]
                    cosine, sine = cos_f[2 * h + j], sin_f[2 * h + j]
                    real = real + (re * cosine - im * sine)
                    imag = imag + (re * sine + im * cosine)
            mids[first + g, 0] = real + pltpu.roll(real, 64, 1)
            mids[first + g, 1] = imag + pltpu.roll(imag, 64, 1)
    loads[4].wait()
    top_tables(angle_mid, cos_t, sin_t)
    low = lax.broadcasted_iota(jnp.int32, (64, 128), 1) < 64
    top = [0.0, 0.0]
    for first in range(0, 4, TOP_GROUP):
        chunks = [
            jnp.where(low, mids[2 * pair, c], mids[2 * pair + 1, c])
            for pair in range(first, first + TOP_GROUP)
            for c in range(2)
        ]
        w_high, w_low = split(jnp.concatenate(chunks, axis=1))
        y = dot(a_top, jnp.concatenate([w_high, w_low, w_high], axis=0))
        y = jnp.concatenate([y[:, 128 * i : 128 * i + 128] for i in range(len(chunks))], axis=0)
        y_high, y_low = split(y)
        z = dot(jnp.concatenate([y_high, y_low, y_high], axis=1), b_top)
        for g in range(TOP_GROUP):
            for j in range(2):
                re = z[256 * g : 256 * g + 128, 128 * j : 128 * j + 128]
                im = z[256 * g + 128 : 256 * g + 256, 128 * j : 128 * j + 128]
                octant = 2 * (first + g) + j
                cosine = cos_t[pl.ds(octant, 128, stride=8), :]
                sine = sin_t[pl.ds(octant, 128, stride=8), :]
                top[0] = top[0] + (re * cosine - im * sine)
                top[1] = top[1] + (re * sine + im * cosine)
    for c in range(2):
        for d in range(16):
            for x in range(2):
                out[16 * x + d, pl.ds(8 * c, 8), :] = top[c][8 * d : 8 * d + 8]


def prepare_kernel(
    angle_fine, angle_mid, theta_mid, phi_mid, theta_top, phi_top,
    cos_f, sin_f, cos_t, sin_t, a_mid, b_mid, a_top, b_top,
):
    fine_tables(angle_fine, cos_f, sin_f)
    top_tables(angle_mid, cos_t, sin_t)
    b_high, b_low = [jnp.concatenate([part, part], axis=0) for part in split(phi_top[...])]
    b_top[...] = jnp.concatenate([b_high, b_high, b_low], axis=1)
    a_top[...] = theta_down(
        theta_top[...], lambda r, c: c == 2 * (r % 32) + r // 32, lambda r, c: r == c
    )
    b_high, b_low = block_diagonal(phi_mid[...], 4)
    b_mid[...] = jnp.concatenate([b_high, b_high, b_low], axis=1)
    a_mid[...] = theta_down(
        theta_mid[...],
        lambda r, c: c == 4 * (r % 8) + r // 8,
        lambda r, c: r == 2 * (c % 32) + c // 32,
    )


def down_kernel(
    parent, fine_oct, mid_oct, cos_f, sin_f, cos_t, sin_t, a_mid, b_mid, a_top, b_top,
    out_hbm, fine_inv, mid_inv, out, sems,
):
    stores = []
    invert(fine_oct, fine_inv, 64, 0)
    invert(mid_oct, mid_inv, 8, lax.axis_index("dir") * 8)
    field = [
        jnp.concatenate([parent[d, pl.ds(8 * c, 8), :] for d in range(16)], axis=0)
        for c in range(2)
    ]
    across = ((1,), (1,))
    for first in range(0, 8, DOWN_GROUP):
        rows = []
        for octant in range(first, first + DOWN_GROUP):
            cosine = cos_t[pl.ds(octant, 128, stride=8), :]
            sine = sin_t[pl.ds(octant, 128, stride=8), :]
            rows.append(field[0] * cosine + field[1] * sine)
            rows.append(field[1] * cosine - field[0] * sine)
        x_high, x_low = split(jnp.concatenate(rows, axis=0))
        y = dot(jnp.concatenate([x_high, x_low, x_high], axis=1), b_top[...], across)
        y = jnp.concatenate([y[128 * i : 128 * i + 128] for i in range(len(rows))], axis=1)
        y_high, y_low = split(y)
        mid = dot(a_top[...], jnp.concatenate([y_high, y_low, y_high], axis=0))
        rows = []
        for g in range(DOWN_GROUP):
            re, im = mid[:, 256 * g : 256 * g + 128], mid[:, 256 * g + 128 : 256 * g + 256]
            for h in range(2):
                c0, s0 = cos_f[2 * h], sin_f[2 * h]
                c1, s1 = cos_f[2 * h + 1], sin_f[2 * h + 1]
                rows.append(jnp.concatenate([re * c0 + im * s0, re * c1 + im * s1], axis=1))
                rows.append(jnp.concatenate([im * c0 - re * s0, im * c1 - re * s1], axis=1))
        x_high, x_low = split(jnp.concatenate(rows, axis=0))
        y = dot(jnp.concatenate([x_high, x_low, x_high], axis=1), b_mid[...], across)
        y = jnp.concatenate([y[64 * i : 64 * i + 64] for i in range(len(rows))], axis=1)
        y_high, y_low = split(y)
        w = dot(a_mid[...], jnp.concatenate([y_high, y_low, y_high], axis=0))
        for g in range(DOWN_GROUP):
            m = mid_inv[first + g]
            for h in range(2):
                boxes = [fine_inv[m * 8 + 4 * h + b] for b in range(4)]
                for c in range(2):
                    lanes = 128 * (4 * g + 2 * h + c)
                    v = group_transpose(
                        [w[8 * i : 8 * i + 8, lanes : lanes + 128] for i in range(4)]
                    )
                    for b in range(4):
                        out[boxes[b], pl.ds(c, 8, stride=2), :] = v[b]
            group = pl.ds(m * 8, 8)
            stores.append(
                pltpu.make_async_copy(out.at[group], out_hbm.at[group], sems.at[first + g])
            )
            stores[-1].start()
    for store in stores:
        store.wait()


def in_vmem(x):
    return pltpu.with_memory_space_constraint(x, pltpu.VMEM)


INVERSES = [pltpu.SMEM((64,), jnp.int32), pltpu.SMEM((8,), jnp.int32)]
TABLES = [((4, 64, 128), F32)] * 2 + [((1024, 128), F32)] * 2
DOWN_MATRICES = [((32, 192), BF16), ((128, 768), BF16), ((64, 384), BF16), ((128, 384), BF16)]


def call_up(fine, fine_oct, mid_oct, tables_of):
    return pl.pallas_call(
        up_kernel,
        out_shape=pltpu.VMEM((32, 16, 128), F32),
        in_specs=[ANY] * 9,
        out_specs=VMEM,
        scratch_shapes=INVERSES
        + [pltpu.VMEM(*table) for table in TABLES]
        + [
            pltpu.VMEM((8, 2, 64, 128), F32),
            pltpu.VMEM((64, 16, 128), F32),
            pltpu.SMEM((64,), jnp.int32),
            pltpu.SMEM((128,), jnp.int32),
            pltpu.VMEM((256, 128), F32),
            pltpu.VMEM((1024, 128), F32),
            pltpu.VMEM((32, 64), F32),
            pltpu.VMEM((32, 64), F32),
            pltpu.VMEM((64, 128), F32),
            pltpu.VMEM((64, 128), F32),
            pltpu.SemaphoreType.DMA((9,)),
        ],
        name="upward",
    )(fine, fine_oct, mid_oct, *tables_of)


def call_prepare(tables_of):
    shapes = TABLES + DOWN_MATRICES
    return pl.pallas_call(
        prepare_kernel,
        out_shape=[pltpu.VMEM(*shape) for shape in shapes],
        in_specs=[VMEM] * 6,
        out_specs=[VMEM] * len(shapes),
        cost_estimate=pl.CostEstimate(flops=200000000, bytes_accessed=2000000, transcendentals=0),
        compiler_params=pltpu.CompilerParams(vmem_limit_bytes=12 * 2**20),
        name="prepare",
    )(*tables_of)


def call_down(parent, fine_oct, mid_oct, prepared):
    return pl.pallas_call(
        down_kernel,
        out_shape=jax.ShapeDtypeStruct((64, 16, 128), F32),
        in_specs=[VMEM, SMEM, SMEM] + [VMEM] * 8,
        out_specs=ANY,
        scratch_shapes=INVERSES
        + [pltpu.VMEM((64, 16, 128), F32), pltpu.SemaphoreType.DMA((8,))],
        compiler_params=pltpu.CompilerParams(vmem_limit_bytes=24 * 2**20),
        name="downward",
    )(in_vmem(parent), fine_oct, mid_oct, *[in_vmem(x) for x in prepared])


def add_pairs(slots, tables, fields, t, total):
    real, imag = [total[0]] + [0.0] * 3, [total[1]] + [0.0] * 3
    for k in range(32):
        fr, fi = [
            sum(field[slot[t, k], pl.ds(8 * c, 8), :] for slot, field in zip(slots, fields))
            for c in range(2)
        ]
        tr = tables[32 * t + k, pl.ds(0, 8, stride=2), :]
        ti = tables[32 * t + k, pl.ds(1, 8, stride=2), :]
        real[k % 4] = real[k % 4] + (fr * tr - fi * ti)
        imag[k % 4] = imag[k % 4] + (fr * ti + fi * tr)
    return (real[0] + real[1]) + (real[2] + real[3]), (imag[0] + imag[1]) + (imag[2] + imag[3])


def first_kernel(
    slots0, slots1, slots2, operator, fields0, fields1, fields2,
    tables, out, listed0, listed1, listed2, sems, slot_sems,
):
    listed, fields = (listed0, listed1, listed2), (fields0, fields1, fields2)
    lists = [
        pltpu.make_async_copy(source, target, slot_sems.at[i])
        for i, (source, target) in enumerate(zip((slots0, slots1, slots2), listed))
    ]
    loads = [
        pltpu.make_async_copy(
            operator.at[pl.ds(32 * t, 32)], tables.at[pl.ds(32 * t, 32)], sems.at[t]
        )
        for t in range(16)
    ]
    for copy in lists + loads:
        copy.start()
    for copy in lists:
        copy.wait()
    for t in range(16):
        loads[t].wait()
        real, imag = add_pairs(listed, tables, fields, t, (0.0, 0.0))
        out[t, pl.ds(0, 8), :] = real
        out[t, pl.ds(8, 8), :] = imag


def last_kernel(slots, tables, fields, partial, out):
    for t in range(16):
        total = partial[t, pl.ds(0, 8), :], partial[t, pl.ds(8, 8), :]
        real, imag = add_pairs((slots,), tables, (fields,), t, total)
        out[t, pl.ds(0, 8), :] = real
        out[t, pl.ds(8, 8), :] = imag


def call_first(slots, operator, fields):
    return pl.pallas_call(
        first_kernel,
        out_shape=[pltpu.VMEM((512, 16, 128), F32), pltpu.VMEM((16, 16, 128), F32)],
        in_specs=[ANY] * 3 + [pl.BlockSpec(memory_space=pltpu.HBM)] + [VMEM] * 3,
        out_specs=[VMEM, VMEM],
        scratch_shapes=[pltpu.SMEM((16, 32), jnp.int32)] * 3
        + [pltpu.SemaphoreType.DMA((16,)), pltpu.SemaphoreType.DMA((3,))],
        cost_estimate=pl.CostEstimate(flops=200000000, bytes_accessed=6000000, transcendentals=0),
        compiler_params=pltpu.CompilerParams(vmem_limit_bytes=8 * 2**20),
        name="first",
    )(
        *slots,
        pltpu.with_memory_space_constraint(operator, pltpu.HBM),
        *[in_vmem(field) for field in fields],
    )


def call_last(slots, tables, fields, partial):
    return pl.pallas_call(
        last_kernel,
        out_shape=pltpu.VMEM((16, 16, 128), F32),
        in_specs=[SMEM, VMEM, VMEM, VMEM],
        out_specs=VMEM,
        compiler_params=pltpu.CompilerParams(vmem_limit_bytes=6 * 2**20),
        name="last",
    )(slots, in_vmem(tables), in_vmem(fields), in_vmem(partial))


def permutations():
    place = lambda x, y, core: x * 16 + (y % 8) * 2 + core
    every = [(x, y, core) for x in range(2) for y in range(8) for core in range(2)]
    ring = lambda by: [(place(x, y, c), place(x, y + (by, -by)[c], 1 - c)) for x, y, c in every]
    other = [(place(x, y, c), place(x, y, 1 - c)) for x, y, c in every]
    return ring(1), ring(-1), other


def gather_tops(own):
    first, second, other = permutations()
    send = lambda x, perm: lax.ppermute(x, "sub", perm)
    zero = jnp.zeros_like(own[:1])
    up, down = [], []
    a = b = own
    for _ in range(3):
        a, b = send(b, first), send(a, second)
        up.append(a)
        down.append(b)
    half = own.shape[0] // 2
    fourth_a = send(b[:half], first)
    fourth_b = send(a[half:], second)
    early = jnp.concatenate([own, up[0], up[1], down[1], down[0], zero], axis=0)
    early_far = send(early, other)
    late = jnp.concatenate([up[2], fourth_a, fourth_b, down[2], zero], axis=0)
    late_far = send(late, other)
    return early, late, early_far, late_far


def slots_of(boxes, my_sub):
    sub, slot = boxes // 16, boxes % 16
    rise = (sub // 2 - my_sub // 2) % 8
    holder = (sub + rise) % 2
    step = jnp.where(holder == 0, rise, (8 - rise) % 8)
    far = holder != my_sub % 2
    late = (step >= 3) & (step <= 5)
    place = jnp.where(step >= 3, step - 3, step) * 32 + (sub // 16) * 16 + slot
    early_slots = [jnp.where((far == side) & ~late, place, 160) for side in (False, True)]
    late_slots = [jnp.where((far == side) & late, place, 96) for side in (False, True)]
    return early_slots[0], late_slots[0], early_slots[1], late_slots[1]


def body(
    fine_fields,
    fine_octant,
    mid_octant,
    shift_fine,
    shift_mid,
    interp_theta_mid,
    interp_phi_mid,
    interp_theta_top,
    interp_phi_top,
    partners,
    translation,
):
    my_sub = lax.axis_index("sub")
    fine = fine_fields.reshape(64, 2, 8, 128).transpose(0, 2, 1, 3).reshape(64, 16, 128)
    operator = translation.reshape(512, 2, 8, 128).transpose(0, 2, 1, 3).reshape(512, 16, 128)
    tables_of = (
        shift_fine.reshape(8, 32, 128).transpose(1, 0, 2).reshape(256, 128),
        shift_mid.reshape(8, 128, 128).transpose(1, 0, 2).reshape(1024, 128),
        interp_theta_mid.T,
        interp_phi_mid.T,
        interp_theta_top.T,
        interp_phi_top.T,
    )
    slots = slots_of(partners, my_sub)
    top = call_up(fine, fine_octant, mid_octant, tables_of)
    prepared = call_prepare(tables_of)
    pairs = [
        [(x * 16 + i) * 16 + d for x in range(2) for d in range(16)] for i in range(16)
    ]
    own = lax.all_to_all(
        top, ("sub", "dir"), split_axis=0, concat_axis=0, tiled=True, axis_index_groups=pairs
    )
    fields = gather_tops(own)
    tables, partial = call_first(slots[:3], operator, fields[:3])
    incoming = call_last(slots[3], tables, fields[3], partial)
    parent = lax.all_to_all(incoming, "dir", split_axis=0, concat_axis=0, tiled=True)
    result = call_down(parent, fine_octant, mid_octant, prepared)
    return result.reshape(64, 8, 2, 128).transpose(0, 2, 1, 3).reshape(64, 2, 1024)


def solution(mesh):
    in_specs = (
        P(("sub", "dir"), None, None),
        P(("sub", "dir")),
        P("sub"),
        P(),
        P(),
        P(),
        P(),
        P(),
        P(),
        P("sub", None),
        P("sub", None, None, "dir"),
    )
    out_specs = P(("sub", "dir"), None, None)
    return jax.shard_map(body, mesh=mesh, in_specs=in_specs, out_specs=out_specs, check_vma=False)
```

```python
import jax
import jax.numpy as jnp
from jax import lax
from jax.experimental import pallas as pl
from jax.experimental.pallas import tpu as pltpu
from jax.sharding import PartitionSpec as P


F32 = jnp.float32
BF16 = jnp.bfloat16
VMEM = pl.BlockSpec(memory_space=pltpu.VMEM)
SMEM = pl.BlockSpec(memory_space=pltpu.SMEM)
UP_GROUP, TOP_GROUP, DOWN_GROUP = 4, 2, 4
ANY = pl.BlockSpec(memory_space=pl.ANY)


def split(x):
    high = x.astype(BF16)
    return high, (x - high.astype(F32)).astype(BF16)


def dot(a, b, dims=((1,), (0,))):
    return lax.dot_general(a, b, (dims, ((), ())), preferred_element_type=F32)


def onehot(shape, source):
    rows = lax.broadcasted_iota(jnp.int32, shape, 0)
    cols = lax.broadcasted_iota(jnp.int32, shape, 1)
    return jnp.where(source(rows, cols), 1.0, 0.0).astype(BF16)


def cos_sin(angles):
    half = angles * 0.5
    square = half * half
    sine = -1.0 / 39916800.0
    for term in (1.0 / 362880.0, -1.0 / 5040.0, 1.0 / 120.0, -1.0 / 6.0, 1.0):
        sine = sine * square + term
    sine = sine * half
    cosine = 1.0 / 479001600.0
    for term in (-1.0 / 3628800.0, 1.0 / 40320.0, -1.0 / 720.0, 1.0 / 24.0, -0.5, 1.0):
        cosine = cosine * square + term
    return 1.0 - 2.0 * (sine * sine), 2.0 * (sine * cosine)


def group_transpose(v):
    lane = lax.broadcasted_iota(jnp.int32, v[0].shape, 1)
    low = lane < 64
    even = (lane // 32) % 2 == 0
    roll = lambda x, by: pltpu.roll(x, by, 1)
    x0 = jnp.where(low, v[0], roll(v[2], 64))
    x2 = jnp.where(low, roll(v[0], 64), v[2])
    x1 = jnp.where(low, v[1], roll(v[3], 64))
    x3 = jnp.where(low, roll(v[1], 64), v[3])
    return [
        jnp.where(even, x0, roll(x1, 32)),
        jnp.where(even, roll(x0, 96), x1),
        jnp.where(even, x2, roll(x3, 32)),
        jnp.where(even, roll(x2, 96), x3),
    ]


def invert(octants, inverse, count, first):
    def step(i, _):
        inverse[(i // 8) * 8 + octants[first + i]] = i
        return 0

    lax.fori_loop(0, count, step, 0, unroll=8)


def fine_tables(angle_ref, cos_ref, sin_ref):
    for pair in range(4):
        first = angle_ref[pl.ds(2 * pair, 32, stride=8), :]
        second = angle_ref[pl.ds(2 * pair + 1, 32, stride=8), :]
        low = lax.broadcasted_iota(jnp.int32, first.shape, 1) < 64
        for odd, angles in enumerate(
            (
                jnp.where(low, first, pltpu.roll(second, 64, 1)),
                jnp.where(low, pltpu.roll(first, 64, 1), second),
            )
        ):
            cosine, sine = cos_sin(angles)
            cos_ref[pair, pl.ds(32 * odd, 32), :] = cosine
            sin_ref[pair, pl.ds(32 * odd, 32), :] = sine


def top_tables(angle_ref, cos_ref, sin_ref):
    for i in range(16):
        cosine, sine = cos_sin(angle_ref[pl.ds(64 * i, 64), :])
        cos_ref[pl.ds(64 * i, 64), :] = cosine
        sin_ref[pl.ds(64 * i, 64), :] = sine


def block_diagonal(matrix, copies):
    n, k = matrix.shape
    spread = onehot((k, copies * k), lambda r, c: c % k == r)
    out = []
    for part in split(matrix):
        wide = dot(part, spread)
        tall = jnp.concatenate([wide] * copies, axis=0)
        rows = lax.broadcasted_iota(jnp.int32, tall.shape, 0) // n
        cols = lax.broadcasted_iota(jnp.int32, tall.shape, 1) // k
        out.append(jnp.where(rows == cols, tall, 0.0).astype(BF16))
    return out


def theta_up(theta, rows, cols):
    targets, sources = theta.shape[1], theta.shape[0]
    high, low = [
        dot(onehot((targets, targets), rows), part, ((1,), (1,))).astype(BF16)
        for part in split(theta)
    ]
    wide = (sources, 3 * sources)
    order = lambda r, c: cols(r, c % sources)
    first = onehot(wide, lambda r, c: order(r, c) & (c < 2 * sources))
    last = onehot(wide, lambda r, c: order(r, c) & (c >= 2 * sources))
    return (dot(high, first) + dot(low, last)).astype(BF16)


def theta_down(theta, rows, cols):
    sources, targets = theta.shape
    high, low = [
        dot(onehot((sources, sources), rows), part).astype(BF16) for part in split(theta)
    ]
    wide = (targets, 3 * targets)
    order = lambda r, c: cols(r, c % targets)
    first = onehot(wide, lambda r, c: order(r, c) & (c < 2 * targets))
    last = onehot(wide, lambda r, c: order(r, c) & (c >= 2 * targets))
    return (dot(high, first) + dot(low, last)).astype(BF16)


def up_kernel(*refs):
    sources, (out, fine_inv, mid_inv, cos_f, sin_f, cos_t, sin_t, mids) = refs[:9], refs[9:17]
    targets, sems = refs[17:26], refs[26]
    loads = [
        pltpu.make_async_copy(source, target, sems.at[i])
        for i, (source, target) in enumerate(zip(sources, targets))
    ]
    fine, fine_oct, mid_oct, angle_fine, angle_mid, theta_mid, phi_mid, theta_top, phi_top = targets
    for i in (5, 6, 7, 8, 3, 1, 2, 0, 4):
        loads[i].start()
    for i in (5, 6, 7, 8):
        loads[i].wait()
    a_mid = theta_up(
        theta_mid[...],
        lambda r, c: c == 2 * (r % 32) + r // 32,
        lambda r, c: r == 4 * (c % 8) + c // 8,
    )
    a_top = theta_up(
        theta_top[...], lambda r, c: r == c, lambda r, c: r == 2 * (c % 32) + c // 32
    )
    b_high, b_low = block_diagonal(phi_mid[...], 4)
    b_mid = jnp.concatenate([b_high, b_high, b_low], axis=0)
    b_high, b_low = block_diagonal(phi_top[...], 2)
    b_top = jnp.concatenate([b_high, b_high, b_low], axis=0)
    loads[3].wait()
    fine_tables(angle_fine, cos_f, sin_f)
    loads[1].wait()
    loads[2].wait()
    invert(fine_oct, fine_inv, 64, 0)
    invert(mid_oct, mid_inv, 8, lax.axis_index("dir") * 8)
    loads[0].wait()
    for first in range(0, 8, UP_GROUP):
        chunks = []
        for octant in range(first, first + UP_GROUP):
            m = mid_inv[octant]
            for h in range(2):
                boxes = [fine_inv[m * 8 + 4 * h + b] for b in range(4)]
                for c in range(2):
                    v = [fine[box, pl.ds(c, 8, stride=2), :] for box in boxes]
                    chunks.append(jnp.concatenate(group_transpose(v), axis=0))
        w_high, w_low = split(jnp.concatenate(chunks, axis=1))
        y = dot(a_mid, jnp.concatenate([w_high, w_low, w_high], axis=0))
        y = jnp.concatenate([y[:, 128 * i : 128 * i + 128] for i in range(len(chunks))], axis=0)
        y_high, y_low = split(y)
        z = dot(jnp.concatenate([y_high, y_low, y_high], axis=1), b_mid)
        for g in range(UP_GROUP):
            real, imag = 0.0, 0.0
            for h in range(2):
                row = 256 * g + 128 * h
                for j in range(2):
                    re = z[row : row + 64, 128 * j : 128 * j + 128]
                    im = z[row + 64 : row + 128, 128 * j : 128 * j + 128]
                    cosine, sine = cos_f[2 * h + j], sin_f[2 * h + j]
                    real = real + (re * cosine - im * sine)
                    imag = imag + (re * sine + im * cosine)
            mids[first + g, 0] = real + pltpu.roll(real, 64, 1)
            mids[first + g, 1] = imag + pltpu.roll(imag, 64, 1)
    loads[4].wait()
    top_tables(angle_mid, cos_t, sin_t)
    low = lax.broadcasted_iota(jnp.int32, (64, 128), 1) < 64
    top = [0.0, 0.0]
    for first in range(0, 4, TOP_GROUP):
        chunks = [
            jnp.where(low, mids[2 * pair, c], mids[2 * pair + 1, c])
            for pair in range(first, first + TOP_GROUP)
            for c in range(2)
        ]
        w_high, w_low = split(jnp.concatenate(chunks, axis=1))
        y = dot(a_top, jnp.concatenate([w_high, w_low, w_high], axis=0))
        y = jnp.concatenate([y[:, 128 * i : 128 * i + 128] for i in range(len(chunks))], axis=0)
        y_high, y_low = split(y)
        z = dot(jnp.concatenate([y_high, y_low, y_high], axis=1), b_top)
        for g in range(TOP_GROUP):
            for j in range(2):
                re = z[256 * g : 256 * g + 128, 128 * j : 128 * j + 128]
                im = z[256 * g + 128 : 256 * g + 256, 128 * j : 128 * j + 128]
                octant = 2 * (first + g) + j
                cosine = cos_t[pl.ds(octant, 128, stride=8), :]
                sine = sin_t[pl.ds(octant, 128, stride=8), :]
                top[0] = top[0] + (re * cosine - im * sine)
                top[1] = top[1] + (re * sine + im * cosine)
    for c in range(2):
        for d in range(16):
            for x in range(2):
                out[16 * x + d, pl.ds(8 * c, 8), :] = top[c][8 * d : 8 * d + 8]


def prepare_kernel(
    angle_fine, angle_mid, theta_mid, phi_mid, theta_top, phi_top,
    cos_f, sin_f, cos_t, sin_t, a_mid, b_mid, a_top, b_top,
):
    fine_tables(angle_fine, cos_f, sin_f)
    top_tables(angle_mid, cos_t, sin_t)
    b_high, b_low = [jnp.concatenate([part, part], axis=0) for part in split(phi_top[...])]
    b_top[...] = jnp.concatenate([b_high, b_high, b_low], axis=1)
    a_top[...] = theta_down(
        theta_top[...], lambda r, c: c == 2 * (r % 32) + r // 32, lambda r, c: r == c
    )
    b_high, b_low = block_diagonal(phi_mid[...], 4)
    b_mid[...] = jnp.concatenate([b_high, b_high, b_low], axis=1)
    a_mid[...] = theta_down(
        theta_mid[...],
        lambda r, c: c == 4 * (r % 8) + r // 8,
        lambda r, c: r == 2 * (c % 32) + c // 32,
    )


def down_kernel(
    parent, fine_oct, mid_oct, cos_f, sin_f, cos_t, sin_t, a_mid, b_mid, a_top, b_top,
    out_hbm, fine_inv, mid_inv, out, sems,
):
    stores = []
    invert(fine_oct, fine_inv, 64, 0)
    invert(mid_oct, mid_inv, 8, lax.axis_index("dir") * 8)
    field = [
        jnp.concatenate([parent[d, pl.ds(8 * c, 8), :] for d in range(16)], axis=0)
        for c in range(2)
    ]
    across = ((1,), (1,))
    for first in range(0, 8, DOWN_GROUP):
        rows = []
        for octant in range(first, first + DOWN_GROUP):
            cosine = cos_t[pl.ds(octant, 128, stride=8), :]
            sine = sin_t[pl.ds(octant, 128, stride=8), :]
            rows.append(field[0] * cosine + field[1] * sine)
            rows.append(field[1] * cosine - field[0] * sine)
        x_high, x_low = split(jnp.concatenate(rows, axis=0))
        y = dot(jnp.concatenate([x_high, x_low, x_high], axis=1), b_top[...], across)
        y = jnp.concatenate([y[128 * i : 128 * i + 128] for i in range(len(rows))], axis=1)
        y_high, y_low = split(y)
        mid = dot(a_top[...], jnp.concatenate([y_high, y_low, y_high], axis=0))
        rows = []
        for g in range(DOWN_GROUP):
            re, im = mid[:, 256 * g : 256 * g + 128], mid[:, 256 * g + 128 : 256 * g + 256]
            for h in range(2):
                c0, s0 = cos_f[2 * h], sin_f[2 * h]
                c1, s1 = cos_f[2 * h + 1], sin_f[2 * h + 1]
                rows.append(jnp.concatenate([re * c0 + im * s0, re * c1 + im * s1], axis=1))
                rows.append(jnp.concatenate([im * c0 - re * s0, im * c1 - re * s1], axis=1))
        x_high, x_low = split(jnp.concatenate(rows, axis=0))
        y = dot(jnp.concatenate([x_high, x_low, x_high], axis=1), b_mid[...], across)
        y = jnp.concatenate([y[64 * i : 64 * i + 64] for i in range(len(rows))], axis=1)
        y_high, y_low = split(y)
        w = dot(a_mid[...], jnp.concatenate([y_high, y_low, y_high], axis=0))
        for g in range(DOWN_GROUP):
            m = mid_inv[first + g]
            for h in range(2):
                boxes = [fine_inv[m * 8 + 4 * h + b] for b in range(4)]
                for c in range(2):
                    lanes = 128 * (4 * g + 2 * h + c)
                    v = group_transpose(
                        [w[8 * i : 8 * i + 8, lanes : lanes + 128] for i in range(4)]
                    )
                    for b in range(4):
                        out[boxes[b], pl.ds(c, 8, stride=2), :] = v[b]
            group = pl.ds(m * 8, 8)
            stores.append(
                pltpu.make_async_copy(out.at[group], out_hbm.at[group], sems.at[first + g])
            )
            stores[-1].start()
    for store in stores:
        store.wait()


def in_vmem(x):
    return pltpu.with_memory_space_constraint(x, pltpu.VMEM)


INVERSES = [pltpu.SMEM((64,), jnp.int32), pltpu.SMEM((8,), jnp.int32)]
TABLES = [((4, 64, 128), F32)] * 2 + [((1024, 128), F32)] * 2
DOWN_MATRICES = [((32, 192), BF16), ((128, 768), BF16), ((64, 384), BF16), ((128, 384), BF16)]


def call_up(fine, fine_oct, mid_oct, tables_of):
    return pl.pallas_call(
        up_kernel,
        out_shape=pltpu.VMEM((32, 16, 128), F32),
        in_specs=[ANY] * 9,
        out_specs=VMEM,
        scratch_shapes=INVERSES
        + [pltpu.VMEM(*table) for table in TABLES]
        + [
            pltpu.VMEM((8, 2, 64, 128), F32),
            pltpu.VMEM((64, 16, 128), F32),
            pltpu.SMEM((64,), jnp.int32),
            pltpu.SMEM((128,), jnp.int32),
            pltpu.VMEM((256, 128), F32),
            pltpu.VMEM((1024, 128), F32),
            pltpu.VMEM((32, 64), F32),
            pltpu.VMEM((32, 64), F32),
            pltpu.VMEM((64, 128), F32),
            pltpu.VMEM((64, 128), F32),
            pltpu.SemaphoreType.DMA((9,)),
        ],
        name="upward",
    )(fine, fine_oct, mid_oct, *tables_of)


def call_prepare(tables_of):
    shapes = TABLES + DOWN_MATRICES
    return pl.pallas_call(
        prepare_kernel,
        out_shape=[pltpu.VMEM(*shape) for shape in shapes],
        in_specs=[VMEM] * 6,
        out_specs=[VMEM] * len(shapes),
        cost_estimate=pl.CostEstimate(flops=200000000, bytes_accessed=2000000, transcendentals=0),
        compiler_params=pltpu.CompilerParams(vmem_limit_bytes=12 * 2**20),
        name="prepare",
    )(*tables_of)


def call_down(parent, fine_oct, mid_oct, prepared):
    return pl.pallas_call(
        down_kernel,
        out_shape=jax.ShapeDtypeStruct((64, 16, 128), F32),
        in_specs=[VMEM, SMEM, SMEM] + [VMEM] * 8,
        out_specs=ANY,
        scratch_shapes=INVERSES
        + [pltpu.VMEM((64, 16, 128), F32), pltpu.SemaphoreType.DMA((8,))],
        compiler_params=pltpu.CompilerParams(vmem_limit_bytes=24 * 2**20),
        name="downward",
    )(in_vmem(parent), fine_oct, mid_oct, *[in_vmem(x) for x in prepared])


def add_pairs(slots, tables, fields, t, total):
    real, imag = [total[0]] + [0.0] * 3, [total[1]] + [0.0] * 3
    for k in range(32):
        fr, fi = [
            sum(field[slot[t, k], pl.ds(8 * c, 8), :] for slot, field in zip(slots, fields))
            for c in range(2)
        ]
        tr = tables[32 * t + k, pl.ds(0, 8, stride=2), :]
        ti = tables[32 * t + k, pl.ds(1, 8, stride=2), :]
        real[k % 4] = real[k % 4] + (fr * tr - fi * ti)
        imag[k % 4] = imag[k % 4] + (fr * ti + fi * tr)
    return (real[0] + real[1]) + (real[2] + real[3]), (imag[0] + imag[1]) + (imag[2] + imag[3])


def first_kernel(
    slots0, slots1, slots2, operator, fields0, fields1, fields2,
    tables, out, listed0, listed1, listed2, sems, slot_sems,
):
    listed, fields = (listed0, listed1, listed2), (fields0, fields1, fields2)
    lists = [
        pltpu.make_async_copy(source, target, slot_sems.at[i])
        for i, (source, target) in enumerate(zip((slots0, slots1, slots2), listed))
    ]
    loads = [
        pltpu.make_async_copy(
            operator.at[pl.ds(32 * t, 32)], tables.at[pl.ds(32 * t, 32)], sems.at[t]
        )
        for t in range(16)
    ]
    for copy in lists + loads:
        copy.start()
    for copy in lists:
        copy.wait()
    for t in range(16):
        loads[t].wait()
        real, imag = add_pairs(listed, tables, fields, t, (0.0, 0.0))
        out[t, pl.ds(0, 8), :] = real
        out[t, pl.ds(8, 8), :] = imag


def last_kernel(slots, tables, fields, partial, out):
    for t in range(16):
        total = partial[t, pl.ds(0, 8), :], partial[t, pl.ds(8, 8), :]
        real, imag = add_pairs((slots,), tables, (fields,), t, total)
        out[t, pl.ds(0, 8), :] = real
        out[t, pl.ds(8, 8), :] = imag


def call_first(slots, operator, fields):
    return pl.pallas_call(
        first_kernel,
        out_shape=[pltpu.VMEM((512, 16, 128), F32), pltpu.VMEM((16, 16, 128), F32)],
        in_specs=[ANY] * 3 + [pl.BlockSpec(memory_space=pltpu.HBM)] + [VMEM] * 3,
        out_specs=[VMEM, VMEM],
        scratch_shapes=[pltpu.SMEM((16, 32), jnp.int32)] * 3
        + [pltpu.SemaphoreType.DMA((16,)), pltpu.SemaphoreType.DMA((3,))],
        cost_estimate=pl.CostEstimate(flops=200000000, bytes_accessed=6000000, transcendentals=0),
        compiler_params=pltpu.CompilerParams(vmem_limit_bytes=8 * 2**20),
        name="first",
    )(
        *slots,
        pltpu.with_memory_space_constraint(operator, pltpu.HBM),
        *[in_vmem(field) for field in fields],
    )


def call_last(slots, tables, fields, partial):
    return pl.pallas_call(
        last_kernel,
        out_shape=pltpu.VMEM((16, 16, 128), F32),
        in_specs=[SMEM, VMEM, VMEM, VMEM],
        out_specs=VMEM,
        compiler_params=pltpu.CompilerParams(vmem_limit_bytes=6 * 2**20),
        name="last",
    )(slots, in_vmem(tables), in_vmem(fields), in_vmem(partial))


def permutations():
    place = lambda x, y, core: x * 16 + (y % 8) * 2 + core
    every = [(x, y, core) for x in range(2) for y in range(8) for core in range(2)]
    ring = lambda by: [(place(x, y, c), place(x, y + (by, -by)[c], 1 - c)) for x, y, c in every]
    other = [(place(x, y, c), place(x, y, 1 - c)) for x, y, c in every]
    return ring(1), ring(-1), other


def gather_tops(own):
    first, second, other = permutations()
    send = lambda x, perm: lax.ppermute(x, "sub", perm)
    zero = jnp.zeros_like(own[:1])
    up, down = [], []
    a = b = own
    for _ in range(3):
        a, b = send(b, first), send(a, second)
        up.append(a)
        down.append(b)
    fourth = send(b, first)
    early = jnp.concatenate([own, up[0], up[1], down[1], down[0], zero], axis=0)
    early_far = send(early, other)
    late = jnp.concatenate([up[2], fourth, down[2], zero], axis=0)
    late_far = send(late, other)
    return early, late, early_far, late_far


def slots_of(boxes, my_sub):
    sub, slot = boxes // 16, boxes % 16
    rise = (sub // 2 - my_sub // 2) % 8
    holder = (sub + rise) % 2
    step = jnp.where(holder == 0, rise, (8 - rise) % 8)
    far = holder != my_sub % 2
    late = (step >= 3) & (step <= 5)
    place = jnp.where(step >= 3, step - 3, step) * 32 + (sub // 16) * 16 + slot
    early_slots = [jnp.where((far == side) & ~late, place, 160) for side in (False, True)]
    late_slots = [jnp.where((far == side) & late, place, 96) for side in (False, True)]
    return early_slots[0], late_slots[0], early_slots[1], late_slots[1]


def body(
    fine_fields,
    fine_octant,
    mid_octant,
    shift_fine,
    shift_mid,
    interp_theta_mid,
    interp_phi_mid,
    interp_theta_top,
    interp_phi_top,
    partners,
    translation,
):
    my_sub = lax.axis_index("sub")
    fine = fine_fields.reshape(64, 2, 8, 128).transpose(0, 2, 1, 3).reshape(64, 16, 128)
    operator = translation.reshape(512, 2, 8, 128).transpose(0, 2, 1, 3).reshape(512, 16, 128)
    tables_of = (
        shift_fine.reshape(8, 32, 128).transpose(1, 0, 2).reshape(256, 128),
        shift_mid.reshape(8, 128, 128).transpose(1, 0, 2).reshape(1024, 128),
        interp_theta_mid.T,
        interp_phi_mid.T,
        interp_theta_top.T,
        interp_phi_top.T,
    )
    slots = slots_of(partners, my_sub)
    top = call_up(fine, fine_octant, mid_octant, tables_of)
    prepared = call_prepare(tables_of)
    pairs = [
        [(x * 16 + i) * 16 + d for x in range(2) for d in range(16)] for i in range(16)
    ]
    own = lax.all_to_all(
        top, ("sub", "dir"), split_axis=0, concat_axis=0, tiled=True, axis_index_groups=pairs
    )
    fields = gather_tops(own)
    tables, partial = call_first(slots[:3], operator, fields[:3])
    incoming = call_last(slots[3], tables, fields[3], partial)
    parent = lax.all_to_all(incoming, "dir", split_axis=0, concat_axis=0, tiled=True)
    result = call_down(parent, fine_octant, mid_octant, prepared)
    return result.reshape(64, 8, 2, 128).transpose(0, 2, 1, 3).reshape(64, 2, 1024)


def solution(mesh):
    in_specs = (
        P(("sub", "dir"), None, None),
        P(("sub", "dir")),
        P("sub"),
        P(),
        P(),
        P(),
        P(),
        P(),
        P(),
        P("sub", None),
        P("sub", None, None, "dir"),
    )
    out_specs = P(("sub", "dir"), None, None)
    return jax.shard_map(body, mesh=mesh, in_specs=in_specs, out_specs=out_specs, check_vma=False)
```
